256 devices in a mesh: node: 32 (over y, x, core), head: 8 (over z).
Axes of the slice: x: 4, y: 4, z: 8, core: 2. Of those that a mesh axis runs over, the one named last changes fastest.
Arguments:
- features: bfloat16 [65536, 100], P('node'), may hold values from -6 to 6
- proj_weight: bfloat16 [100, 512], P(None, 'head'), may hold values from -0.625 to 0.625
- score_src: float32 [8, 64], P('head'), may hold values from -150 to 150
- score_dst: float32 [8, 64], P('head'), may hold values from -0.75 to 0.75
- request_rows: int32 [32, 32, 256], P('node'), may hold values from 0 to 2047
- slot_index: int32 [16384, 16], P('node'), may hold values from 0 to 8191
- slot_count: int32 [16384], P('node'), may hold values from 1 to 16
- out_weight: bfloat16 [512, 512], replicated, may hold values from -0.25 to 0.25
Outputs:
- layer_out: bfloat16 [16384, 512], P(('node', 'head'))
The draws below stay inside these ranges and needn't reach their ends.
All inputs are finite; a program needn't handle non-finite values.
Results may differ from the reference program's by a relative error of at most 0.012.
The reference program's roundings to bfloat16 on the way count: a program that leaves them out, or rounds other values in their place, can miss the bound.
Values may be sent and summed in bfloat16 or wider, within the bound.
A program may use at most 64 MiB of HBM per device.

```python
import math
import jax
import jax.numpy as jnp
import numpy as np
from jax import lax

FEAT = 100
HEADS = 8
HEAD_DIM = 64
D_OUT = 512
SLOTS = 16
NODE_DEV = 2048
DST_DEV = 512
CAP = 256
NODES = 65536
DESTS = 16384
N_NODE = 32


def draw_score_src(key, part):
    base = jax.random.normal(jax.random.fold_in(key, 11), (HEADS, HEAD_DIM), jnp.float32)
    base = jnp.clip(base, -4.0, 4.0) / math.sqrt(HEAD_DIM)
    return jnp.clip(base, -150.0, 150.0)


def plant(values, rng, least, high):
    longest = values.shape.index(max(values.shape))
    spots = []
    for shift in (0, 1):
        where = [jax.random.randint(jax.random.fold_in(rng, axis), (), 0, length) for axis, length in enumerate(values.shape)]
        where[longest] = (where[longest] + shift) % values.shape[longest]
        spots.append(tuple(where))
    return values.at[spots[0]].set(least).at[spots[1]].set(high)


def block_scale(stream_key, shape, shards, low, largest):
    level = 1.0
    for position, parts in shards:
        heights = jax.random.uniform(jax.random.fold_in(jax.random.fold_in(stream_key, 6), position), (parts,), jnp.float32, low / len(shards), largest / len(shards))
        level = level * jnp.repeat(jnp.exp(heights), shape[position] // parts).reshape((-1,) + (1,) * (len(shape) - 1 - position))
    return level


def cumulative_ranks(amount, slope):
    weights = [(1 << 20) // math.isqrt(standing ** slope) + 1 for standing in range(1, amount + 1)]
    spread = 1 + sum(weights) // (1 << 30)
    return np.cumsum(np.array([max(1, weight // spread) for weight in weights]))


def ranked(key, shape, number_of, skew):
    table = cumulative_ranks(number_of, skew)
    ticket = jax.random.randint(jax.random.fold_in(key, 1), shape, 0, int(table[number_of - 1]))
    standing = jnp.searchsorted(jnp.asarray(table, jnp.int32), ticket, side="right")
    return jax.random.permutation(jax.random.fold_in(key, 2), number_of)[standing].astype(jnp.int32)


def gaussian(key, shape, deviation, bound, pieces=(), kind=jnp.bfloat16):
    values = jax.random.normal(key, shape, jnp.float32) * deviation
    if len(pieces) > 0:
        values = block_scale(key, shape, pieces, -0.22, 0.18) * values
    return jnp.clip(values, min=-bound, max=bound).astype(kind)


def setup_inputs(seed: int = 0) -> dict:
    key_of = jax.random.split(jax.random.key(seed), 9)
    return {
        "features": gaussian(key_of[0], (NODES, FEAT), 1.0, 6.0, ((0, 32),)),
        "proj_weight": gaussian(key_of[1], (FEAT, HEADS * HEAD_DIM), FEAT ** -0.5, 0.625, ((1, 8),)),
        "score_src": draw_score_src(jax.random.fold_in(key_of[8], 71), 0),
        "score_dst": gaussian(key_of[3], (HEADS, HEAD_DIM), HEAD_DIM ** -0.5, 0.75, ((0, 8),), jnp.float32),
        "request_rows": plant(jax.random.randint(key_of[4], (N_NODE, N_NODE, CAP), 0, NODE_DEV), jax.random.fold_in(key_of[4], 1), 0, NODE_DEV - 1).astype(jnp.int32),
        "slot_index": plant(ranked(key_of[5], (DESTS, SLOTS), N_NODE * CAP, 1), jax.random.fold_in(key_of[5], 3), 0, (N_NODE * CAP) - 1).astype(jnp.int32),
        "slot_count": plant(jax.random.randint(key_of[6], (DESTS,), 1, SLOTS + 1), jax.random.fold_in(key_of[6], 1), 1, SLOTS).astype(jnp.int32),
        "out_weight": gaussian(key_of[7], (HEADS * HEAD_DIM, D_OUT), (HEADS * HEAD_DIM) ** -0.5, 0.25),
    }


def reference(features, proj_weight, score_src, score_dst, request_rows, slot_index, slot_count, out_weight):
    flat_requests = request_rows.reshape(N_NODE, N_NODE * CAP)
    owner_dev = (slot_index // CAP).astype(jnp.int32)
    device_of = (jnp.arange(DESTS, dtype=jnp.int32) // DST_DEV).astype(jnp.int32)
    local_row = flat_requests[device_of[:, None], slot_index]
    neighbour = (owner_dev * NODE_DEV + local_row).astype(jnp.int32)

    def one_block(pair):
        ids, counts = pair
        picked = features[ids.reshape(-1)]
        zvals = jnp.dot(picked, proj_weight, preferred_element_type=jnp.float32).astype(jnp.bfloat16)
        zfloat = zvals.astype(jnp.float32).reshape(DST_DEV, SLOTS, HEADS, HEAD_DIM)
        src_part = jnp.einsum("rshd,hd->rsh", zfloat, score_src.astype(jnp.float32))
        dst_part = jnp.einsum("rhd,hd->rh", zfloat[:, 0], score_dst.astype(jnp.float32))
        logit = src_part + dst_part[:, None, :]
        logit = jnp.where(logit > 0, logit, 0.2 * logit)
        live_mask = (jnp.arange(SLOTS, dtype=jnp.int32)[None, :] < counts[:, None])[:, :, None]
        logit = jnp.where(live_mask, logit, -1e30)
        peak = jnp.max(logit, axis=1, keepdims=True)
        weights = jnp.where(live_mask, jnp.exp(logit - peak), 0.0)
        alpha = (weights / jnp.sum(weights, axis=1, keepdims=True)).astype(jnp.bfloat16)
        summed = jnp.einsum("rsh,rshd->rhd", alpha.astype(jnp.float32), zfloat)
        hidden = jax.nn.elu(summed).astype(jnp.bfloat16).reshape(DST_DEV, HEADS * HEAD_DIM)
        return jnp.dot(hidden, out_weight, preferred_element_type=jnp.float32).astype(jnp.bfloat16)

    result = lax.map(one_block, (neighbour.reshape(N_NODE, DST_DEV, SLOTS), slot_count.reshape(N_NODE, DST_DEV)))
    return result.reshape(DESTS, D_OUT)
```

```python
import functools

import jax
import jax.numpy as jnp
from jax import lax
from jax.experimental import pallas as pl
from jax.experimental.pallas import tpu as pltpu
from jax.sharding import PartitionSpec as P

MESH = pl.DeviceIdType.MESH
RING = (0, 1, 2, 1)
FEAT, HEADS, DIM, OUT, SLOTS = 100, 8, 64, 512, 16
CAP, HALF, QUART = 256, 128, 64
ROWS = 64
OWNERS = 32


def hops(k):
    return RING[k // 8] + RING[(k // 2) % 4]


PEERS = sorted(range(1, OWNERS), key=lambda k: -hops(k))
FAR = [k for k in PEERS if hops(k) >= 2]
NEAR = [k for k in PEERS if hops(k) < 2]


def shifted(k, sign):
    me = lax.axis_index("node")
    y, x, c = me // 8, (me // 2) % 4, me % 2
    dy, dx, dc = k // 8, (k // 2) % 4, k % 2
    return (((y + sign * dy + 4) % 4) * 4 + (x + sign * dx + 4) % 4) * 2 + (c + sign * dc + 2) % 2


def kernel(
    feat_t, w_t, s_src, s_dst, req, slot_t, cnt, ow, out,
    feat, blk, tab, rx, stage, sendbuf, w_all, sc_all, gath, zf, req_sm, own_sm, slot_sm,
    rq_s, rq_r, rw_s, rw_r, up_s, up_r, dn_s, dn_r, w_s, w_r, sc_s, sc_r, loc,
):
    me, h = lax.axis_index("node"), lax.axis_index("head")
    half = h % 2
    up, down = (h + 1) % HEADS, (h + HEADS - 1) % HEADS

    barrier = pltpu.get_barrier_semaphore()
    for k in PEERS:
        pl.semaphore_signal(barrier, inc=1, device_id=(shifted(k, 1), h), device_id_type=MESH)
    for z in range(1, HEADS):
        pl.semaphore_signal(barrier, inc=1, device_id=(me, (h + z) % HEADS), device_id_type=MESH)

    own_copy = pltpu.make_async_copy(req.at[me], own_sm, loc.at[0])
    own_copy.start()
    slot_copy = pltpu.make_async_copy(slot_t, slot_sm, loc.at[1])
    slot_copy.start()

    blk[...] = jnp.zeros_like(blk)
    for j in range(feat.shape[0] // 128):
        blk[0:FEAT, :] = feat_t[:, j * 128 : (j + 1) * 128].astype(jnp.float32)
        feat[j * 128 : (j + 1) * 128, :] = blk[...].T
    both = jnp.concatenate([s_src[...], s_dst[...]], axis=0)
    sc_all[h] = jnp.concatenate([both, both], axis=1)
    w_all[h] = w_t[...]

    pl.semaphore_wait(barrier, OWNERS - 1 + HEADS - 1)

    sends = []
    for k in PEERS:
        owner = shifted(k, -1)
        if k in FAR:
            src, dst = req.at[owner, pl.ds(half * HALF, HALF)], req_sm.at[k, pl.ds(0, HALF)]
        else:
            src, dst = req.at[owner], req_sm.at[k]
        copy = pltpu.make_async_remote_copy(
            src_ref=src, dst_ref=dst, send_sem=rq_s.at[k], recv_sem=rq_r.at[k],
            device_id=(owner, h), device_id_type=MESH,
        )
        copy.start()
        sends.append(copy)
    along = []
    for z in range(1, HEADS):
        peer = (me, (h + z) % HEADS)
        copy = pltpu.make_async_remote_copy(
            src_ref=w_t, dst_ref=w_all.at[h], send_sem=w_s.at[z], recv_sem=w_r.at[z],
            device_id=peer, device_id_type=MESH,
        )
        copy.start()
        along.append(copy)
        copy = pltpu.make_async_remote_copy(
            src_ref=sc_all.at[h], dst_ref=sc_all.at[h], send_sem=sc_s.at[z], recv_sem=sc_r.at[z],
            device_id=peer, device_id_type=MESH,
        )
        copy.start()
        along.append(copy)

    def pick(table, number, target, base, count):
        def some(b, carry):
            first = b * 16
            for u in range(16):
                i = number(first + u)
                target[pl.ds(base + first + u, 1), :] = table[pl.ds(i, 1), :]
            return carry

        lax.fori_loop(0, count // 16, some, 0)

    own_copy.wait()
    pick(feat, lambda i: own_sm[i], tab, me * CAP, CAP)

    pending = None
    for k in PEERS:
        count = HALF if k in FAR else CAP
        if k in FAR:
            src, dst = req.at[0, pl.ds(0, HALF)], req_sm.at[k, pl.ds(0, HALF)]
        else:
            src, dst = req.at[0], req_sm.at[k]
        pltpu.make_async_remote_copy(
            src_ref=src, dst_ref=dst, send_sem=rq_s.at[k], recv_sem=rq_r.at[k],
            device_id=(shifted(k, 1), h), device_id_type=MESH,
        ).wait_recv()
        pick(feat, lambda i, k=k: req_sm[k, i], stage, 0, count)
        sendbuf[k, 0:count, :] = stage[0:count, :].astype(jnp.bfloat16)
        if pending is not None:
            pending.start()
        if k in FAR:
            dst = rx.at[k, pl.ds(half * HALF, HALF)]
        else:
            dst = rx.at[k]
        pending = pltpu.make_async_remote_copy(
            src_ref=sendbuf.at[k, pl.ds(0, count)], dst_ref=dst, send_sem=rw_s.at[k],
            recv_sem=rw_r.at[k], device_id=(shifted(k, 1), h), device_id_type=MESH,
        )
        sends.append(pending)
    pending.start()

    def spread(k, start, count):
        place = pl.multiple_of(shifted(k, -1) * CAP + start, 64)
        tab[pl.ds(place, count), :] = rx[k, pl.ds(pl.multiple_of(start, 64), count), :].astype(
            jnp.float32
        )

    def hand(k, part, mine, first):
        start = mine * HALF + first * QUART
        ref = rx.at[k, pl.ds(start, QUART)]
        sem = (up_s, up_r) if first == 0 else (dn_s, dn_r)
        return pltpu.make_async_remote_copy(
            src_ref=ref, dst_ref=ref, send_sem=sem[0].at[k], recv_sem=sem[1].at[k],
            device_id=(me, part), device_id_type=MESH,
        )

    for k in FAR:
        pltpu.make_async_remote_copy(
            src_ref=sendbuf.at[k, pl.ds(0, HALF)], dst_ref=rx.at[k, pl.ds(half * HALF, HALF)],
            send_sem=rw_s.at[k], recv_sem=rw_r.at[k], device_id=(me, up), device_id_type=MESH,
        ).wait_recv()
        for part, first in ((up, 0), (down, 1)):
            copy = hand(k, part, half, first)
            copy.start()
            along.append(copy)
        spread(k, half * HALF, HALF)
    for k in NEAR:
        pltpu.make_async_remote_copy(
            src_ref=sendbuf.at[k], dst_ref=rx.at[k], send_sem=rw_s.at[k], recv_sem=rw_r.at[k],
            device_id=(me, up), device_id_type=MESH,
        ).wait_recv()
        spread(k, 0, CAP)
    for k in FAR:
        hand(k, down, 1 - half, 0).wait_recv()
        hand(k, up, 1 - half, 1).wait_recv()
        spread(k, (1 - half) * HALF, HALF)
    for z in range(1, HEADS):
        other = (h + HEADS - z) % HEADS
        pltpu.make_async_remote_copy(
            src_ref=w_t, dst_ref=w_all.at[other], send_sem=w_s.at[z], recv_sem=w_r.at[z],
            device_id=(me, up), device_id_type=MESH,
        ).wait_recv()
        pltpu.make_async_remote_copy(
            src_ref=sc_all.at[h], dst_ref=sc_all.at[other], send_sem=sc_s.at[z],
            recv_sem=sc_r.at[z], device_id=(me, up), device_id_type=MESH,
        ).wait_recv()

    slot_copy.wait()
    for s in range(SLOTS):
        pick(tab, lambda i, s=s: slot_sm[s, h * ROWS + i], gath, s * ROWS, ROWS)

    row = lax.broadcasted_iota(jnp.int32, (2 * HEADS, OUT), 0)
    lane = lax.broadcasted_iota(jnp.int32, (2 * HEADS, OUT), 1)
    score = jnp.zeros((2 * HEADS, OUT), jnp.float32)
    for head in range(HEADS):
        for which in range(2):
            vec = sc_all[head, which : which + 1, :]
            vec = jnp.broadcast_to(jnp.concatenate([vec] * 4, axis=1), (2 * HEADS, OUT))
            hit = (row == which * HEADS + head) & (lane // DIM == head)
            score = jnp.where(hit, vec, score)
    top = score.astype(jnp.bfloat16)
    rest = score - top.astype(jnp.float32)
    mid = rest.astype(jnp.bfloat16)
    low = (rest - mid.astype(jnp.float32)).astype(jnp.bfloat16)

    g = gath[...][:, 0:FEAT].astype(jnp.bfloat16)
    for head in range(HEADS):
        zf[head * DIM : (head + 1) * DIM, :] = lax.dot_general(
            w_all[head], g, (((1,), (1,)), ((), ())), preferred_element_type=jnp.float32
        ).astype(jnp.bfloat16)
    z = zf[...]
    parts = [jnp.dot(piece, z, preferred_element_type=jnp.float32) for piece in (top, mid, low)]
    total = parts[0] + parts[1] + parts[2]
    n = SLOTS * ROWS // 128
    lanes = lax.broadcasted_iota(jnp.int32, (HEADS, 128), 1)
    dst_part = total[HEADS:, 0:128]
    dst_part = jnp.where(lanes < ROWS, dst_part, pltpu.roll(dst_part, ROWS, 1))
    pair = cnt[0:1, pl.ds(pl.multiple_of(h // 2 * 128, 128), 128)]
    pair = jnp.broadcast_to(pair, (HEADS, 128))
    turned = pltpu.roll(pair, ROWS, 1)
    counts = jnp.where((lanes // ROWS) == half, pair, turned)
    logits, lives = [], []
    for j in range(n):
        logit = total[0:HEADS, j * 128 : (j + 1) * 128] + dst_part
        logit = jnp.where(logit > 0, logit, 0.2 * logit)
        live = (2 * j + lanes // ROWS) < counts
        logits.append(jnp.where(live, logit, -1e30))
        lives.append(live)
    peak = functools.reduce(jnp.maximum, logits)
    peak = jnp.maximum(peak, pltpu.roll(peak, ROWS, 1))
    weights = [
        jnp.where(live, jnp.exp(logit - peak), 0.0) for live, logit in zip(lives, logits)
    ]
    norm = functools.reduce(jnp.add, weights)
    norm = norm + pltpu.roll(norm, ROWS, 1)
    alphas = [(w / norm).astype(jnp.bfloat16).astype(jnp.float32) for w in weights]
    hidden = []
    for head in range(HEADS):
        acc = jnp.zeros((DIM, 128), jnp.float32)
        for j in range(n):
            part = zf[head * DIM : (head + 1) * DIM, j * 128 : (j + 1) * 128].astype(jnp.float32)
            acc = acc + part * jnp.broadcast_to(alphas[j][head : head + 1, :], (DIM, 128))
        acc = acc + pltpu.roll(acc, ROWS, 1)
        hidden.append(jnp.where(acc > 0, acc, jnp.exp(jnp.minimum(acc, 0.0)) - 1.0))
    hidden = jnp.concatenate(hidden, axis=0)
    hidden = hidden.T[0:ROWS, :].astype(jnp.bfloat16)
    out[...] = jnp.dot(hidden, ow[...], preferred_element_type=jnp.float32).astype(jnp.bfloat16)

    for copy in sends + along:
        copy.wait_send()


def local(
    features, proj_weight, score_src, score_dst, request_rows, slot_index, slot_count, out_weight
):
    vmem = pl.BlockSpec(memory_space=pltpu.VMEM)
    dma = pltpu.SemaphoreType.DMA
    nodes = features.shape[0]
    return pl.pallas_call(
        kernel,
        out_shape=jax.ShapeDtypeStruct((ROWS, OUT), jnp.bfloat16),
        in_specs=[vmem] * 8,
        out_specs=vmem,
        scratch_shapes=[
            pltpu.VMEM((nodes, 128), jnp.float32),
            pltpu.VMEM((128, 128), jnp.float32),
            pltpu.VMEM((OWNERS * CAP, 128), jnp.float32),
            pltpu.VMEM((OWNERS, CAP, 128), jnp.bfloat16),
            pltpu.VMEM((CAP, 128), jnp.float32),
            pltpu.VMEM((OWNERS, CAP, 128), jnp.bfloat16),
            pltpu.VMEM((HEADS, DIM, FEAT), jnp.bfloat16),
            pltpu.VMEM((HEADS, 2, 128), jnp.float32),
            pltpu.VMEM((SLOTS * ROWS, 128), jnp.float32),
            pltpu.VMEM((OUT, SLOTS * ROWS), jnp.bfloat16),
            pltpu.SMEM((OWNERS, CAP), jnp.int32),
            pltpu.SMEM((CAP,), jnp.int32),
            pltpu.SMEM((SLOTS, 512), jnp.int32),
        ]
        + [dma((OWNERS,))] * 8
        + [dma((HEADS,))] * 4
        + [dma((2,))],
        compiler_params=pltpu.CompilerParams(
            collective_id=0, has_side_effects=True, vmem_limit_bytes=48 * 1024 * 1024
        ),
        name="layer",
    )(
        features.T, proj_weight.T, score_src, score_dst, request_rows.reshape(OWNERS, CAP),
        slot_index.T, slot_count.reshape(1, -1), out_weight,
    )


def solution(mesh):
    in_specs = (
        P("node", None),
        P(None, "head"),
        P("head", None),
        P("head", None),
        P("node", None, None),
        P("node", None),
        P("node"),
        P(),
    )
    out_specs = P(("node", "head"), None)
    return jax.shard_map(local, mesh=mesh, in_specs=in_specs, out_specs=out_specs, check_vma=False)
```

```python
import functools

import jax
import jax.numpy as jnp
from jax import lax
from jax.experimental import pallas as pl
from jax.experimental.pallas import tpu as pltpu
from jax.sharding import PartitionSpec as P

MESH = pl.DeviceIdType.MESH
RING = (0, 1, 2, 1)
FEAT, HEADS, DIM, OUT, SLOTS = 100, 8, 64, 512, 16
CAP, HALF, QUART = 256, 128, 64
ROWS = 64
OWNERS = 32


def hops(k):
    return RING[k // 8] + RING[(k // 2) % 4]


PEERS = sorted(range(1, OWNERS), key=lambda k: -hops(k))
FAR = [k for k in PEERS if hops(k) >= 2]
NEAR = [k for k in PEERS if hops(k) < 2]


def shifted(k, sign):
    me = lax.axis_index("node")
    y, x, c = me // 8, (me // 2) % 4, me % 2
    dy, dx, dc = k // 8, (k // 2) % 4, k % 2
    return (((y + sign * dy + 4) % 4) * 4 + (x + sign * dx + 4) % 4) * 2 + (c + sign * dc + 2) % 2


def kernel(
    feat_t, w_t, s_src, s_dst, req, slot_t, cnt, ow, out,
    feat_in, req_in, sc_in, cnt_in, ow_in,
    feat, blk, tab, rx, stage, sendbuf, w_all, sc_all, gath, zf, req_sm, own_sm, slot_sm,
    rq_s, rq_r, rw_s, rw_r, up_s, up_r, dn_s, dn_r, w_s, w_r, sc_s, sc_r, loc,
):
    me, h = lax.axis_index("node"), lax.axis_index("head")
    half = h % 2
    up, down = (h + 1) % HEADS, (h + HEADS - 1) % HEADS

    barrier = pltpu.get_barrier_semaphore()
    for k in PEERS:
        pl.semaphore_signal(barrier, inc=1, device_id=(shifted(k, 1), h), device_id_type=MESH)
    for z in range(1, HEADS):
        pl.semaphore_signal(barrier, inc=1, device_id=(me, (h + z) % HEADS), device_id_type=MESH)

    lane_block = pl.multiple_of(h // 2 * 128, 128)
    loads = [
        pltpu.make_async_copy(src, dst, loc.at[n])
        for n, (src, dst) in enumerate(
            (
                (feat_t, feat_in),
                (req, req_in),
                (req.at[me, pl.ds(0, HALF)], own_sm.at[0]),
                (req.at[me, pl.ds(HALF, HALF)], own_sm.at[1]),
                (w_t, w_all.at[h]),
                (s_src, sc_in.at[0]),
                (s_dst, sc_in.at[1]),
                (slot_t.at[:, pl.ds(lane_block, 128)], slot_sm),
                (cnt.at[:, pl.ds(lane_block, 128)], cnt_in),
                (ow, ow_in),
            )
        )
    ]
    for load in loads:
        load.start()
    feat_load, req_load, own_load, own_load2, w_load, src_load, dst_load, slot_load, cnt_load, ow_load = loads

    blk[...] = jnp.zeros_like(blk)
    feat_load.wait()
    for j in range(feat.shape[0] // 128):
        blk[0:FEAT, :] = feat_in[:, j * 128 : (j + 1) * 128].astype(jnp.float32)
        feat[j * 128 : (j + 1) * 128, :] = blk[...].T
    src_load.wait()
    dst_load.wait()
    both = jnp.concatenate([sc_in[0], sc_in[1]], axis=0)
    sc_all[h] = jnp.concatenate([both, both], axis=1)
    w_load.wait()
    req_load.wait()

    pl.semaphore_wait(barrier, OWNERS - 1 + HEADS - 1)

    def ask(k, part, owner, target):
        column = half if k in FAR else part
        return pltpu.make_async_remote_copy(
            src_ref=req_in.at[owner, pl.ds(pl.multiple_of(column * HALF, HALF), HALF)],
            dst_ref=req_sm.at[k, part],
            send_sem=rq_s.at[k, part], recv_sem=rq_r.at[k, part],
            device_id=(target, h), device_id_type=MESH,
        )

    sends = []
    for k in PEERS:
        owner = shifted(k, -1)
        for part in range(1 if k in FAR else 2):
            copy = ask(k, part, owner, owner)
            copy.start()
            sends.append(copy)
    along = []
    for z in range(1, HEADS):
        peer = (me, (h + z) % HEADS)
        copy = pltpu.make_async_remote_copy(
            src_ref=w_all.at[h], dst_ref=w_all.at[h], send_sem=w_s.at[z], recv_sem=w_r.at[z],
            device_id=peer, device_id_type=MESH,
        )
        copy.start()
        along.append(copy)
        copy = pltpu.make_async_remote_copy(
            src_ref=sc_all.at[h], dst_ref=sc_all.at[h], send_sem=sc_s.at[z], recv_sem=sc_r.at[z],
            device_id=peer, device_id_type=MESH,
        )
        copy.start()
        along.append(copy)

    def pick(table, number, target, base, count):
        for u in range(count):
            target[pl.ds(base + u, 1), :] = table[pl.ds(number(u), 1), :]

    own_load.wait()
    own_load2.wait()

    def own(part, carry):
        pick(feat, lambda u: own_sm[part, u], tab, me * CAP + part * HALF, HALF)
        return carry

    lax.fori_loop(0, 2, own, 0)

    pending = None
    for k in PEERS:
        count = HALF if k in FAR else CAP
        for part in range(count // HALF):
            ask(k, part, 0, shifted(k, 1)).wait_recv()

        def some(part, carry, k=k):
            pick(feat, lambda u: req_sm[k, part, u], stage, part * HALF, HALF)
            return carry

        lax.fori_loop(0, count // HALF, some, 0)
        sendbuf[k, 0:count, :] = stage[0:count, :].astype(jnp.bfloat16)
        if pending is not None:
            pending.start()
        if k in FAR:
            dst = rx.at[k, pl.ds(half * HALF, HALF)]
        else:
            dst = rx.at[k]
        pending = pltpu.make_async_remote_copy(
            src_ref=sendbuf.at[k, pl.ds(0, count)], dst_ref=dst, send_sem=rw_s.at[k],
            recv_sem=rw_r.at[k], device_id=(shifted(k, 1), h), device_id_type=MESH,
        )
        sends.append(pending)
    pending.start()

    def spread(k, start, count):
        place = pl.multiple_of(shifted(k, -1) * CAP + start, 64)
        tab[pl.ds(place, count), :] = rx[k, pl.ds(pl.multiple_of(start, 64), count), :].astype(
            jnp.float32
        )

    def hand(k, part, mine, first):
        start = mine * HALF + first * QUART
        ref = rx.at[k, pl.ds(start, QUART)]
        sem = (up_s, up_r) if first == 0 else (dn_s, dn_r)
        return pltpu.make_async_remote_copy(
            src_ref=ref, dst_ref=ref, send_sem=sem[0].at[k], recv_sem=sem[1].at[k],
            device_id=(me, part), device_id_type=MESH,
        )

    for k in FAR:
        pltpu.make_async_remote_copy(
            src_ref=sendbuf.at[k, pl.ds(0, HALF)], dst_ref=rx.at[k, pl.ds(half * HALF, HALF)],
            send_sem=rw_s.at[k], recv_sem=rw_r.at[k], device_id=(me, up), device_id_type=MESH,
        ).wait_recv()
        for part, first in ((up, 0), (down, 1)):
            copy = hand(k, part, half, first)
            copy.start()
            along.append(copy)
        spread(k, half * HALF, HALF)
    for k in NEAR:
        pltpu.make_async_remote_copy(
            src_ref=sendbuf.at[k], dst_ref=rx.at[k], send_sem=rw_s.at[k], recv_sem=rw_r.at[k],
            device_id=(me, up), device_id_type=MESH,
        ).wait_recv()
        spread(k, 0, CAP)
    for k in FAR:
        hand(k, down, 1 - half, 0).wait_recv()
        hand(k, up, 1 - half, 1).wait_recv()
        spread(k, (1 - half) * HALF, HALF)
    for z in range(1, HEADS):
        other = (h + HEADS - z) % HEADS
        pltpu.make_async_remote_copy(
            src_ref=w_all.at[h], dst_ref=w_all.at[other], send_sem=w_s.at[z], recv_sem=w_r.at[z],
            device_id=(me, up), device_id_type=MESH,
        ).wait_recv()
        pltpu.make_async_remote_copy(
            src_ref=sc_all.at[h], dst_ref=sc_all.at[other], send_sem=sc_s.at[z],
            recv_sem=sc_r.at[z], device_id=(me, up), device_id_type=MESH,
        ).wait_recv()

    slot_load.wait()
    for side in range(2):

        @pl.when(half == side)
        def _(side=side):
            def some(s, carry):
                pick(tab, lambda u: slot_sm[s, side * ROWS + u], gath, s * ROWS, ROWS)
                return carry

            lax.fori_loop(0, SLOTS, some, 0)

    row = lax.broadcasted_iota(jnp.int32, (2 * HEADS, OUT), 0)
    lane = lax.broadcasted_iota(jnp.int32, (2 * HEADS, OUT), 1)
    score = jnp.zeros((2 * HEADS, OUT), jnp.float32)
    for head in range(HEADS):
        for which in range(2):
            vec = sc_all[head, which : which + 1, :]
            vec = jnp.broadcast_to(jnp.concatenate([vec] * 4, axis=1), (2 * HEADS, OUT))
            hit = (row == which * HEADS + head) & (lane // DIM == head)
            score = jnp.where(hit, vec, score)
    top = score.astype(jnp.bfloat16)
    rest = score - top.astype(jnp.float32)
    mid = rest.astype(jnp.bfloat16)
    low = (rest - mid.astype(jnp.float32)).astype(jnp.bfloat16)

    g = gath[...][:, 0:FEAT].astype(jnp.bfloat16)
    for head in range(HEADS):
        zf[head * DIM : (head + 1) * DIM, :] = lax.dot_general(
            w_all[head], g, (((1,), (1,)), ((), ())), preferred_element_type=jnp.float32
        ).astype(jnp.bfloat16)
    z = zf[...]
    parts = [jnp.dot(piece, z, preferred_element_type=jnp.float32) for piece in (top, mid, low)]
    total = parts[0] + parts[1] + parts[2]
    n = SLOTS * ROWS // 128
    lanes = lax.broadcasted_iota(jnp.int32, (HEADS, 128), 1)
    dst_part = total[HEADS:, 0:128]
    dst_part = jnp.where(lanes < ROWS, dst_part, pltpu.roll(dst_part, ROWS, 1))
    cnt_load.wait()
    pair = jnp.broadcast_to(cnt_in[...], (HEADS, 128))
    turned = pltpu.roll(pair, ROWS, 1)
    counts = jnp.where((lanes // ROWS) == half, pair, turned)
    logits, lives = [], []
    for j in range(n):
        logit = total[0:HEADS, j * 128 : (j + 1) * 128] + dst_part
        logit = jnp.where(logit > 0, logit, 0.2 * logit)
        live = (2 * j + lanes // ROWS) < counts
        logits.append(jnp.where(live, logit, -1e30))
        lives.append(live)
    peak = functools.reduce(jnp.maximum, logits)
    peak = jnp.maximum(peak, pltpu.roll(peak, ROWS, 1))
    weights = [
        jnp.where(live, jnp.exp(logit - peak), 0.0) for live, logit in zip(lives, logits)
    ]
    norm = functools.reduce(jnp.add, weights)
    norm = norm + pltpu.roll(norm, ROWS, 1)
    alphas = [(w / norm).astype(jnp.bfloat16).astype(jnp.float32) for w in weights]
    hidden = []
    for head in range(HEADS):
        acc = jnp.zeros((DIM, 128), jnp.float32)
        for j in range(n):
            part = zf[head * DIM : (head + 1) * DIM, j * 128 : (j + 1) * 128].astype(jnp.float32)
            acc = acc + part * jnp.broadcast_to(alphas[j][head : head + 1, :], (DIM, 128))
        acc = acc + pltpu.roll(acc, ROWS, 1)
        hidden.append(jnp.where(acc > 0, acc, jnp.exp(jnp.minimum(acc, 0.0)) - 1.0))
    hidden = jnp.concatenate(hidden, axis=0)
    hidden = hidden.T[0:ROWS, :].astype(jnp.bfloat16)
    ow_load.wait()
    out[...] = jnp.dot(hidden, ow_in[...], preferred_element_type=jnp.float32).astype(jnp.bfloat16)

    for copy in sends + along:
        copy.wait_send()


def local(
    features, proj_weight, score_src, score_dst, request_rows, slot_index, slot_count, out_weight
):
    vmem = pl.BlockSpec(memory_space=pltpu.VMEM)
    dma = pltpu.SemaphoreType.DMA
    nodes = features.shape[0]
    return pl.pallas_call(
        kernel,
        out_shape=jax.ShapeDtypeStruct((ROWS, OUT), jnp.bfloat16),
        in_specs=[pl.BlockSpec(memory_space=pltpu.HBM)] * 8,
        out_specs=vmem,
        scratch_shapes=[
            pltpu.VMEM((FEAT, nodes), jnp.bfloat16),
            pltpu.VMEM((OWNERS, CAP), jnp.int32),
            pltpu.VMEM((2, 1, DIM), jnp.float32),
            pltpu.VMEM((1, 128), jnp.int32),
            pltpu.VMEM((OUT, OUT), jnp.bfloat16),
            pltpu.VMEM((nodes, 128), jnp.float32),
            pltpu.VMEM((128, 128), jnp.float32),
            pltpu.VMEM((OWNERS * CAP, 128), jnp.float32),
            pltpu.VMEM((OWNERS, CAP, 128), jnp.bfloat16),
            pltpu.VMEM((CAP, 128), jnp.float32),
            pltpu.VMEM((OWNERS, CAP, 128), jnp.bfloat16),
            pltpu.VMEM((HEADS, DIM, FEAT), jnp.bfloat16),
            pltpu.VMEM((HEADS, 2, 128), jnp.float32),
            pltpu.VMEM((SLOTS * ROWS, 128), jnp.float32),
            pltpu.VMEM((OUT, SLOTS * ROWS), jnp.bfloat16),
            pltpu.SMEM((OWNERS, 2, HALF), jnp.int32),
            pltpu.SMEM((2, HALF), jnp.int32),
            pltpu.SMEM((SLOTS, 128), jnp.int32),
        ]
        + [dma((OWNERS, 2))] * 2
        + [dma((OWNERS,))] * 6
        + [dma((HEADS,))] * 4
        + [dma((10,))],
        compiler_params=pltpu.CompilerParams(
            collective_id=0, has_side_effects=True, vmem_limit_bytes=60 * 1024 * 1024
        ),
        name="layer",
    )(
        features.T, proj_weight.T, score_src, score_dst, request_rows.reshape(OWNERS, CAP),
        slot_index.T, slot_count.reshape(1, -1), out_weight,
    )


def solution(mesh):
    in_specs = (
        P("node", None),
        P(None, "head"),
        P("head", None),
        P("head", None),
        P("node", None, None),
        P("node", None),
        P("node"),
        P(),
    )
    out_specs = P(("node", "head"), None)
    return jax.shard_map(local, mesh=mesh, in_specs=in_specs, out_specs=out_specs, check_vma=False)
```

```python
import functools

import jax
import jax.numpy as jnp
from jax import lax
from jax.experimental import pallas as pl
from jax.experimental.pallas import tpu as pltpu
from jax.sharding import PartitionSpec as P

MESH = pl.DeviceIdType.MESH
RING = (0, 1, 2, 1)
FEAT, HEADS, DIM, OUT, SLOTS = 100, 8, 64, 512, 16
CAP, HALF = 256, 128
PACK = 104
ROWS = 64
OWNERS = 32


def hops(k):
    return RING[k // 8] + RING[(k // 2) % 4]


FAR = sorted((k for k in range(1, OWNERS) if hops(k) >= 2), key=lambda k: -hops(k))
NEAR = [2, 6, 8, 24, 3, 7, 9, 25, 1]
PEERS = FAR + NEAR
HELD = 6


def shifted(k, sign):
    me = lax.axis_index("node")
    y, x, c = me // 8, (me // 2) % 4, me % 2
    dy, dx, dc = k // 8, (k // 2) % 4, k % 2
    return (((y + sign * dy + 4) % 4) * 4 + (x + sign * dx + 4) % 4) * 2 + (c + sign * dc + 2) % 2


def pack(x):
    lane = lax.broadcasted_iota(jnp.int32, (8, 128), 1)
    group = [x[8 * i : 8 * i + 8] for i in range(16)]
    rows = [jnp.where(lane < 64, group[i], pltpu.roll(group[8 + i], 64, 1)) for i in range(8)]
    for i in range(4):
        acc = group[8 + i]
        for q in (0, 1, 3):
            moved = pltpu.roll(group[4 * q + i], (32 * q - 64) % 128, 1)
            acc = jnp.where(lane // 32 == q, moved, acc)
        rows.append(acc)
    acc = group[12]
    for q in range(16):
        if q != 12:
            acc = jnp.where(lane // 8 == q, pltpu.roll(group[q], (8 * q - 96) % 128, 1), acc)
    rows.append(acc)
    return jnp.concatenate(rows, axis=0)


def unpack(y):
    lane = lax.broadcasted_iota(jnp.int32, (8, 128), 1)
    group = [y[8 * i : 8 * i + 8] for i in range(13)]
    rows = []
    for i in range(16):
        first = group[i] if i < 8 else pltpu.roll(group[i - 8], 64, 1)
        second = group[8 + i % 4]
        if i // 4 != 2:
            second = pltpu.roll(second, (64 - 32 * (i // 4)) % 128, 1)
        third = group[12] if i == 12 else pltpu.roll(group[12], (96 - 8 * i) % 128, 1)
        rows.append(jnp.where(lane < 64, first, jnp.where(lane < 96, second, third)))
    return jnp.concatenate(rows, axis=0)


def kernel(
    feat_t, w_t, s_src, s_dst, req, slot_t, cnt, ow, out,
    feat_in, req_in, sc_in, cnt_in, ow_in,
    feat, blk, tab, rx, stage, sendbuf, w_all, sc_all, gath, zf, sc_mat, req_sm, own_sm, slot_sm,
    rq_s, rq_r, rw_s, rw_r, up_s, up_r, dn_s, dn_r, w_s, w_r, sc_s, sc_r, loc,
):
    me, h = lax.axis_index("node"), lax.axis_index("head")
    half = h % 2
    up, down = (h + 1) % HEADS, (h + HEADS - 1) % HEADS

    barrier = pltpu.get_barrier_semaphore()
    for k in PEERS:
        pl.semaphore_signal(barrier, inc=1, device_id=(shifted(k, 1), h), device_id_type=MESH)
    for z in range(1, HEADS):
        pl.semaphore_signal(barrier, inc=1, device_id=(me, (h + z) % HEADS), device_id_type=MESH)

    lane_block = pl.multiple_of(h // 2 * 128, 128)
    loads = [
        pltpu.make_async_copy(src, dst, loc.at[n])
        for n, (src, dst) in enumerate(
            (
                (feat_t, feat_in),
                (req, req_in),
                (req.at[me, pl.ds(0, HALF)], own_sm.at[0]),
                (req.at[me, pl.ds(HALF, HALF)], own_sm.at[1]),
                (w_t, w_all.at[h]),
                (s_src, sc_in.at[0]),
                (s_dst, sc_in.at[1]),
                (slot_t.at[:, pl.ds(lane_block, 128)], slot_sm),
                (cnt.at[:, pl.ds(lane_block, 128)], cnt_in),
                (ow, ow_in),
            )
        )
    ]
    for load in loads:
        load.start()
    feat_load, req_load, own_load, own_load2, w_load, src_load, dst_load, slot_load, cnt_load, ow_load = loads

    blk[...] = jnp.zeros_like(blk)
    feat_load.wait()
    for j in range(feat.shape[0] // 128):
        blk[0:FEAT, :] = feat_in[:, j * 128 : (j + 1) * 128].astype(jnp.float32)
        feat[j * 128 : (j + 1) * 128, :] = blk[...].T
    src_load.wait()
    dst_load.wait()
    both = jnp.concatenate([sc_in[0], sc_in[1]], axis=0)
    sc_all[h] = jnp.concatenate([both, both], axis=1)
    w_load.wait()
    req_load.wait()

    pl.semaphore_wait(barrier, OWNERS - 1 + HEADS - 1)

    def ask(k, part, owner, target):
        column = half if k in FAR else part
        return pltpu.make_async_remote_copy(
            src_ref=req_in.at[owner, pl.ds(pl.multiple_of(column * HALF, HALF), HALF)],
            dst_ref=req_sm.at[k, part],
            send_sem=rq_s.at[k, part], recv_sem=rq_r.at[k, part],
            device_id=(target, h), device_id_type=MESH,
        )

    sends = []
    for k in PEERS:
        owner = shifted(k, -1)
        for part in range(1 if k in FAR else 2):
            copy = ask(k, part, owner, owner)
            copy.start()
            sends.append(copy)
    along = []
    for z in range(1, HEADS):
        peer = (me, (h + z) % HEADS)
        copy = pltpu.make_async_remote_copy(
            src_ref=w_all.at[h], dst_ref=w_all.at[h], send_sem=w_s.at[z], recv_sem=w_r.at[z],
            device_id=peer, device_id_type=MESH,
        )
        copy.start()
        along.append(copy)
        copy = pltpu.make_async_remote_copy(
            src_ref=sc_all.at[h], dst_ref=sc_all.at[h], send_sem=sc_s.at[z], recv_sem=sc_r.at[z],
            device_id=peer, device_id_type=MESH,
        )
        copy.start()
        along.append(copy)

    def pick(table, number, target, base, count):
        for u in range(count):
            target[pl.ds(base + u, 1), :] = table[pl.ds(number(u), 1), :]

    own_load.wait()
    own_load2.wait()

    def own(part, carry):
        pick(feat, lambda u: own_sm[part, u], tab, me * CAP + part * HALF, HALF)
        return carry

    lax.fori_loop(0, 2, own, 0)

    def give(k):
        src, dst = (sendbuf.at[k, 0], rx.at[k, half]) if k in FAR else (sendbuf.at[k], rx.at[k])
        return pltpu.make_async_remote_copy(
            src_ref=src, dst_ref=dst, send_sem=rw_s.at[k],
            recv_sem=rw_r.at[k], device_id=(shifted(k, 1), h), device_id_type=MESH,
        )

    def send(k):
        copy = give(k)
        copy.start()
        sends.append(copy)

    for n, k in enumerate(PEERS):
        count = HALF if k in FAR else CAP
        for part in range(count // HALF):
            ask(k, part, 0, shifted(k, 1)).wait_recv()

        def some(part, carry, k=k):
            pick(feat, lambda u: req_sm[k, part, u], stage, 0, HALF)
            sendbuf[k, part] = pack(stage[...]).astype(jnp.bfloat16)
            return carry

        lax.fori_loop(0, count // HALF, some, 0)
        if 1 <= n <= len(FAR):
            send(PEERS[n - 1])

    def spread(k, part):
        place = pl.multiple_of(shifted(k, -1) * CAP + part * HALF, HALF)
        tab[pl.ds(place, HALF), :] = unpack(rx[k, part].astype(jnp.float32))

    def hand(k, part, mine, first):
        start, count = (0, 48) if first == FAR.index(k) % 2 else (48, PACK - 48)
        ref = rx.at[k, mine, pl.ds(start, count)]
        sem = (up_s, up_r) if first == 0 else (dn_s, dn_r)
        return pltpu.make_async_remote_copy(
            src_ref=ref, dst_ref=ref, send_sem=sem[0].at[k], recv_sem=sem[1].at[k],
            device_id=(me, part), device_id_type=MESH,
        )

    for n, k in enumerate(FAR):
        give(k).wait_recv()
        for part, first in ((up, 0), (down, 1)):
            copy = hand(k, part, half, first)
            copy.start()
            along.append(copy)
        spread(k, half)
        if HELD <= n < HELD + len(NEAR):
            send(NEAR[n - HELD])
    for z in range(1, HEADS):
        other = (h + HEADS - z) % HEADS
        pltpu.make_async_remote_copy(
            src_ref=w_all.at[h], dst_ref=w_all.at[other], send_sem=w_s.at[z], recv_sem=w_r.at[z],
            device_id=(me, up), device_id_type=MESH,
        ).wait_recv()
        pltpu.make_async_remote_copy(
            src_ref=sc_all.at[h], dst_ref=sc_all.at[other], send_sem=sc_s.at[z],
            recv_sem=sc_r.at[z], device_id=(me, up), device_id_type=MESH,
        ).wait_recv()

    row = lax.broadcasted_iota(jnp.int32, (2 * HEADS, OUT), 0)
    lane = lax.broadcasted_iota(jnp.int32, (2 * HEADS, OUT), 1)
    score = jnp.zeros((2 * HEADS, OUT), jnp.float32)
    for head in range(HEADS):
        for which in range(2):
            vec = sc_all[head, which : which + 1, :]
            vec = jnp.broadcast_to(jnp.concatenate([vec] * 4, axis=1), (2 * HEADS, OUT))
            hit = (row == which * HEADS + head) & (lane // DIM == head)
            score = jnp.where(hit, vec, score)
    top = score.astype(jnp.bfloat16)
    rest = score - top.astype(jnp.float32)
    mid = rest.astype(jnp.bfloat16)
    low = (rest - mid.astype(jnp.float32)).astype(jnp.bfloat16)
    for n, piece in enumerate((top, mid, low)):
        sc_mat[n * 2 * HEADS : (n + 1) * 2 * HEADS, :] = piece

    for k in NEAR:
        give(k).wait_recv()

        def both_halves(part, carry, k=k):
            spread(k, part)
            return carry

        lax.fori_loop(0, 2, both_halves, 0)
    for k in FAR:
        hand(k, down, 1 - half, 0).wait_recv()
        hand(k, up, 1 - half, 1).wait_recv()
        spread(k, 1 - half)
    slot_load.wait()
    for side in range(2):

        @pl.when(half == side)
        def _(side=side):
            def some(s, carry):
                pick(tab, lambda u: slot_sm[s, side * ROWS + u], gath, s * ROWS, ROWS)
                return carry

            lax.fori_loop(0, SLOTS, some, 0)

    g = gath[...][:, 0:FEAT].astype(jnp.bfloat16)
    zf[...] = lax.dot_general(
        w_all[...].reshape(OUT, FEAT), g, (((1,), (1,)), ((), ())),
        preferred_element_type=jnp.float32,
    ).astype(jnp.bfloat16)
    parts = jnp.dot(sc_mat[...], zf[...], preferred_element_type=jnp.float32)
    total = parts[0:16] + parts[16:32] + parts[32:48]
    n = SLOTS * ROWS // 128
    lanes = lax.broadcasted_iota(jnp.int32, (HEADS, 128), 1)
    dst_part = total[HEADS:, 0:128]
    dst_part = jnp.where(lanes < ROWS, dst_part, pltpu.roll(dst_part, ROWS, 1))
    cnt_load.wait()
    pair = jnp.broadcast_to(cnt_in[...], (HEADS, 128))
    turned = pltpu.roll(pair, ROWS, 1)
    counts = jnp.where((lanes // ROWS) == half, pair, turned)
    logits, lives = [], []
    for j in range(n):
        logit = total[0:HEADS, j * 128 : (j + 1) * 128] + dst_part
        logit = jnp.where(logit > 0, logit, 0.2 * logit)
        live = (2 * j + lanes // ROWS) < counts
        logits.append(jnp.where(live, logit, -1e30))
        lives.append(live)
    peak = functools.reduce(jnp.maximum, logits)
    peak = jnp.maximum(peak, pltpu.roll(peak, ROWS, 1))
    weights = [
        jnp.where(live, jnp.exp(logit - peak), 0.0) for live, logit in zip(lives, logits)
    ]
    norm = functools.reduce(jnp.add, weights)
    norm = norm + pltpu.roll(norm, ROWS, 1)
    alphas = [(w / norm).astype(jnp.bfloat16).astype(jnp.float32) for w in weights]
    hidden = []
    for head in range(HEADS):
        acc = jnp.zeros((DIM, 128), jnp.float32)
        for j in range(n):
            part = zf[head * DIM : (head + 1) * DIM, j * 128 : (j + 1) * 128].astype(jnp.float32)
            acc = acc + part * jnp.broadcast_to(alphas[j][head : head + 1, :], (DIM, 128))
        acc = acc + pltpu.roll(acc, ROWS, 1)
        hidden.append(jnp.where(acc > 0, acc, jnp.exp(jnp.minimum(acc, 0.0)) - 1.0))
    hidden = jnp.concatenate(hidden, axis=0)
    hidden = hidden.T[0:ROWS, :].astype(jnp.bfloat16)
    ow_load.wait()
    out[...] = jnp.dot(hidden, ow_in[...], preferred_element_type=jnp.float32).astype(jnp.bfloat16)

    for copy in sends + along:
        copy.wait_send()


def local(
    features, proj_weight, score_src, score_dst, request_rows, slot_index, slot_count, out_weight
):
    vmem = pl.BlockSpec(memory_space=pltpu.VMEM)
    dma = pltpu.SemaphoreType.DMA
    nodes = features.shape[0]
    return pl.pallas_call(
        kernel,
        out_shape=jax.ShapeDtypeStruct((ROWS, OUT), jnp.bfloat16),
        in_specs=[pl.BlockSpec(memory_space=pltpu.HBM)] * 8,
        out_specs=vmem,
        scratch_shapes=[
            pltpu.VMEM((FEAT, nodes), jnp.bfloat16),
            pltpu.VMEM((OWNERS, CAP), jnp.int32),
            pltpu.VMEM((2, 1, DIM), jnp.float32),
            pltpu.VMEM((1, 128), jnp.int32),
            pltpu.VMEM((OUT, OUT), jnp.bfloat16),
            pltpu.VMEM((nodes, 128), jnp.float32),
            pltpu.VMEM((128, 128), jnp.float32),
            pltpu.VMEM((OWNERS * CAP, 128), jnp.float32),
            pltpu.VMEM((OWNERS, 2, PACK, 128), jnp.bfloat16),
            pltpu.VMEM((HALF, 128), jnp.float32),
            pltpu.VMEM((OWNERS, 2, PACK, 128), jnp.bfloat16),
            pltpu.VMEM((HEADS, DIM, FEAT), jnp.bfloat16),
            pltpu.VMEM((HEADS, 2, 128), jnp.float32),
            pltpu.VMEM((SLOTS * ROWS, 128), jnp.float32),
            pltpu.VMEM((OUT, SLOTS * ROWS), jnp.bfloat16),
            pltpu.VMEM((6 * HEADS, OUT), jnp.bfloat16),
            pltpu.SMEM((OWNERS, 2, HALF), jnp.int32),
            pltpu.SMEM((2, HALF), jnp.int32),
            pltpu.SMEM((SLOTS, 128), jnp.int32),
        ]
        + [dma((OWNERS, 2))] * 2
        + [dma((OWNERS,))] * 6
        + [dma((HEADS,))] * 4
        + [dma((10,))],
        compiler_params=pltpu.CompilerParams(
            collective_id=0, has_side_effects=True, vmem_limit_bytes=60 * 1024 * 1024
        ),
        name="layer",
    )(
        features.T, proj_weight.T, score_src, score_dst, request_rows.reshape(OWNERS, CAP),
        slot_index.T, slot_count.reshape(1, -1), out_weight,
    )


def solution(mesh):
    in_specs = (
        P("node", None),
        P(None, "head"),
        P("head", None),
        P("head", None),
        P("node", None, None),
        P("node", None),
        P("node"),
        P(),
    )
    out_specs = P(("node", "head"), None)
    return jax.shard_map(local, mesh=mesh, in_specs=in_specs, out_specs=out_specs, check_vma=False)
```

```python
import functools

import jax
import jax.numpy as jnp
from jax import lax
from jax.experimental import pallas as pl
from jax.experimental.pallas import tpu as pltpu
from jax.sharding import PartitionSpec as P

MESH = pl.DeviceIdType.MESH
RING = (0, 1, 2, 1)
FEAT, HEADS, DIM, OUT, SLOTS = 100, 8, 64, 512, 16
CAP, HALF = 256, 128
PACK = 104
ROWS = 64
OWNERS = 32


def hops(k):
    return RING[k // 8] + RING[(k // 2) % 4]


FAR = sorted((k for k in range(1, OWNERS) if hops(k) >= 2), key=lambda k: -hops(k))[::-1]
NEAR = [2, 6, 8, 24, 3, 7, 9, 25, 1]
PEERS = FAR + NEAR
HELD = 0


def shifted(k, sign):
    me = lax.axis_index("node")
    y, x, c = me // 8, (me // 2) % 4, me % 2
    dy, dx, dc = k // 8, (k // 2) % 4, k % 2
    return (((y + sign * dy + 4) % 4) * 4 + (x + sign * dx + 4) % 4) * 2 + (c + sign * dc + 2) % 2


def pack(x):
    lane = lax.broadcasted_iota(jnp.int32, (8, 128), 1)
    group = [x[8 * i : 8 * i + 8] for i in range(16)]
    rows = [jnp.where(lane < 64, group[i], pltpu.roll(group[8 + i], 64, 1)) for i in range(8)]
    for i in range(4):
        acc = group[8 + i]
        for q in (0, 1, 3):
            moved = pltpu.roll(group[4 * q + i], (32 * q - 64) % 128, 1)
            acc = jnp.where(lane // 32 == q, moved, acc)
        rows.append(acc)
    acc = group[12]
    for q in range(16):
        if q != 12:
            acc = jnp.where(lane // 8 == q, pltpu.roll(group[q], (8 * q - 96) % 128, 1), acc)
    rows.append(acc)
    return jnp.concatenate(rows, axis=0)


def unpack(y):
    lane = lax.broadcasted_iota(jnp.int32, (8, 128), 1)
    group = [y[8 * i : 8 * i + 8] for i in range(13)]
    rows = []
    for i in range(16):
        first = group[i] if i < 8 else pltpu.roll(group[i - 8], 64, 1)
        second = group[8 + i % 4]
        if i // 4 != 2:
            second = pltpu.roll(second, (64 - 32 * (i // 4)) % 128, 1)
        third = group[12] if i == 12 else pltpu.roll(group[12], (96 - 8 * i) % 128, 1)
        rows.append(jnp.where(lane < 64, first, jnp.where(lane < 96, second, third)))
    return jnp.concatenate(rows, axis=0)


def kernel(
    feat_t, w_t, s_src, s_dst, req, slot_t, cnt, ow, out,
    feat_in, req_in, sc_in, cnt_in, ow_in,
    feat, blk, tab, rx, stage, sendbuf, w_all, sc_all, gath, zf, sc_mat, req_sm, own_sm, slot_sm,
    rq_s, rq_r, rw_s, rw_r, up_s, up_r, dn_s, dn_r, w_s, w_r, sc_s, sc_r, loc,
):
    me, h = lax.axis_index("node"), lax.axis_index("head")
    half = h % 2
    up, down = (h + 1) % HEADS, (h + HEADS - 1) % HEADS

    barrier = pltpu.get_barrier_semaphore()
    for k in PEERS:
        pl.semaphore_signal(barrier, inc=1, device_id=(shifted(k, 1), h), device_id_type=MESH)
    for z in range(1, HEADS):
        pl.semaphore_signal(barrier, inc=1, device_id=(me, (h + z) % HEADS), device_id_type=MESH)

    lane_block = pl.multiple_of(h // 2 * 128, 128)
    loads = [
        pltpu.make_async_copy(src, dst, loc.at[n])
        for n, (src, dst) in enumerate(
            (
                (feat_t, feat_in),
                (req, req_in),
                (req.at[me, pl.ds(0, HALF)], own_sm.at[0]),
                (req.at[me, pl.ds(HALF, HALF)], own_sm.at[1]),
                (w_t, w_all.at[h]),
                (s_src, sc_in.at[0]),
                (s_dst, sc_in.at[1]),
                (slot_t.at[:, pl.ds(lane_block, 128)], slot_sm),
                (cnt.at[:, pl.ds(lane_block, 128)], cnt_in),
                (ow, ow_in),
            )
        )
    ]
    for load in loads:
        load.start()
    feat_load, req_load, own_load, own_load2, w_load, src_load, dst_load, slot_load, cnt_load, ow_load = loads

    blk[...] = jnp.zeros_like(blk)
    feat_load.wait()
    for j in range(feat.shape[0] // 128):
        blk[0:FEAT, :] = feat_in[:, j * 128 : (j + 1) * 128].astype(jnp.float32)
        feat[j * 128 : (j + 1) * 128, :] = blk[...].T
    src_load.wait()
    dst_load.wait()
    both = jnp.concatenate([sc_in[0], sc_in[1]], axis=0)
    sc_all[h] = jnp.concatenate([both, both], axis=1)
    w_load.wait()
    req_load.wait()

    pl.semaphore_wait(barrier, OWNERS - 1 + HEADS - 1)

    def ask(k, part, owner, target):
        column = half if k in FAR else part
        return pltpu.make_async_remote_copy(
            src_ref=req_in.at[owner, pl.ds(pl.multiple_of(column * HALF, HALF), HALF)],
            dst_ref=req_sm.at[k, part],
            send_sem=rq_s.at[k, part], recv_sem=rq_r.at[k, part],
            device_id=(target, h), device_id_type=MESH,
        )

    sends = []
    for k in PEERS:
        owner = shifted(k, -1)
        for part in range(1 if k in FAR else 2):
            copy = ask(k, part, owner, owner)
            copy.start()
            sends.append(copy)
    along = []
    for z in range(1, HEADS):
        peer = (me, (h + z) % HEADS)
        copy = pltpu.make_async_remote_copy(
            src_ref=w_all.at[h], dst_ref=w_all.at[h], send_sem=w_s.at[z], recv_sem=w_r.at[z],
            device_id=peer, device_id_type=MESH,
        )
        copy.start()
        along.append(copy)
        copy = pltpu.make_async_remote_copy(
            src_ref=sc_all.at[h], dst_ref=sc_all.at[h], send_sem=sc_s.at[z], recv_sem=sc_r.at[z],
            device_id=peer, device_id_type=MESH,
        )
        copy.start()
        along.append(copy)

    def pick(table, number, target, base, count):
        for u in range(count):
            target[pl.ds(base + u, 1), :] = table[pl.ds(number(u), 1), :]

    own_load.wait()
    own_load2.wait()

    def own(part, carry):
        pick(feat, lambda u: own_sm[part, u], tab, me * CAP + part * HALF, HALF)
        return carry

    lax.fori_loop(0, 2, own, 0)

    def give(k):
        src, dst = (sendbuf.at[k, 0], rx.at[k, half]) if k in FAR else (sendbuf.at[k], rx.at[k])
        return pltpu.make_async_remote_copy(
            src_ref=src, dst_ref=dst, send_sem=rw_s.at[k],
            recv_sem=rw_r.at[k], device_id=(shifted(k, 1), h), device_id_type=MESH,
        )

    def send(k):
        copy = give(k)
        copy.start()
        sends.append(copy)

    def serve(k):
        parts = 1 if k in FAR else 2
        for part in range(parts):
            ask(k, part, 0, shifted(k, 1)).wait_recv()

        def some(part, carry):
            pick(feat, lambda u: req_sm[k, part, u], stage, 0, HALF)
            sendbuf[k, part] = pack(stage[...]).astype(jnp.bfloat16)
            return carry

        lax.fori_loop(0, parts, some, 0)
        send(k)

    for k in FAR:
        serve(k)

    def spread(k, part):
        place = pl.multiple_of(shifted(k, -1) * CAP + part * HALF, HALF)
        tab[pl.ds(place, HALF), :] = unpack(rx[k, part].astype(jnp.float32))

    def hand(k, part, mine, first):
        start, count = (0, 48) if first == FAR.index(k) % 2 else (48, PACK - 48)
        ref = rx.at[k, mine, pl.ds(start, count)]
        sem = (up_s, up_r) if first == 0 else (dn_s, dn_r)
        return pltpu.make_async_remote_copy(
            src_ref=ref, dst_ref=ref, send_sem=sem[0].at[k], recv_sem=sem[1].at[k],
            device_id=(me, part), device_id_type=MESH,
        )

    for n, k in enumerate(FAR):
        give(k).wait_recv()
        for part, first in ((up, 0), (down, 1)):
            copy = hand(k, part, half, first)
            copy.start()
            along.append(copy)
        spread(k, half)
        if HELD <= n < HELD + len(NEAR):
            serve(NEAR[n - HELD])
    for z in range(1, HEADS):
        other = (h + HEADS - z) % HEADS
        pltpu.make_async_remote_copy(
            src_ref=w_all.at[h], dst_ref=w_all.at[other], send_sem=w_s.at[z], recv_sem=w_r.at[z],
            device_id=(me, up), device_id_type=MESH,
        ).wait_recv()
        pltpu.make_async_remote_copy(
            src_ref=sc_all.at[h], dst_ref=sc_all.at[other], send_sem=sc_s.at[z],
            recv_sem=sc_r.at[z], device_id=(me, up), device_id_type=MESH,
        ).wait_recv()

    row = lax.broadcasted_iota(jnp.int32, (2 * HEADS, OUT), 0)
    lane = lax.broadcasted_iota(jnp.int32, (2 * HEADS, OUT), 1)
    score = jnp.zeros((2 * HEADS, OUT), jnp.float32)
    for head in range(HEADS):
        for which in range(2):
            vec = sc_all[head, which : which + 1, :]
            vec = jnp.broadcast_to(jnp.concatenate([vec] * 4, axis=1), (2 * HEADS, OUT))
            hit = (row == which * HEADS + head) & (lane // DIM == head)
            score = jnp.where(hit, vec, score)
    top = score.astype(jnp.bfloat16)
    rest = score - top.astype(jnp.float32)
    mid = rest.astype(jnp.bfloat16)
    low = (rest - mid.astype(jnp.float32)).astype(jnp.bfloat16)
    for n, piece in enumerate((top, mid, low)):
        sc_mat[n * 2 * HEADS : (n + 1) * 2 * HEADS, :] = piece

    for k in NEAR:
        give(k).wait_recv()

        def both_halves(part, carry, k=k):
            spread(k, part)
            return carry

        lax.fori_loop(0, 2, both_halves, 0)
    for k in FAR:
        hand(k, down, 1 - half, 0).wait_recv()
        hand(k, up, 1 - half, 1).wait_recv()
        spread(k, 1 - half)
    slot_load.wait()
    for side in range(2):

        @pl.when(half == side)
        def _(side=side):
            def some(s, carry):
                pick(tab, lambda u: slot_sm[s, side * ROWS + u], gath, s * ROWS, ROWS)
                return carry

            lax.fori_loop(0, SLOTS, some, 0)

    g = gath[...][:, 0:FEAT].astype(jnp.bfloat16)
    zf[...] = lax.dot_general(
        w_all[...].reshape(OUT, FEAT), g, (((1,), (1,)), ((), ())),
        preferred_element_type=jnp.float32,
    ).astype(jnp.bfloat16)
    parts = jnp.dot(sc_mat[...], zf[...], preferred_element_type=jnp.float32)
    total = parts[0:16] + parts[16:32] + parts[32:48]
    n = SLOTS * ROWS // 128
    lanes = lax.broadcasted_iota(jnp.int32, (HEADS, 128), 1)
    dst_part = total[HEADS:, 0:128]
    dst_part = jnp.where(lanes < ROWS, dst_part, pltpu.roll(dst_part, ROWS, 1))
    cnt_load.wait()
    pair = jnp.broadcast_to(cnt_in[...], (HEADS, 128))
    turned = pltpu.roll(pair, ROWS, 1)
    counts = jnp.where((lanes // ROWS) == half, pair, turned)
    logits, lives = [], []
    for j in range(n):
        logit = total[0:HEADS, j * 128 : (j + 1) * 128] + dst_part
        logit = jnp.where(logit > 0, logit, 0.2 * logit)
        live = (2 * j + lanes // ROWS) < counts
        logits.append(jnp.where(live, logit, -1e30))
        lives.append(live)
    peak = functools.reduce(jnp.maximum, logits)
    peak = jnp.maximum(peak, pltpu.roll(peak, ROWS, 1))
    weights = [
        jnp.where(live, jnp.exp(logit - peak), 0.0) for live, logit in zip(lives, logits)
    ]
    norm = functools.reduce(jnp.add, weights)
    norm = norm + pltpu.roll(norm, ROWS, 1)
    alphas = [(w / norm).astype(jnp.bfloat16).astype(jnp.float32) for w in weights]
    hidden = []
    for head in range(HEADS):
        acc = jnp.zeros((DIM, 128), jnp.float32)
        for j in range(n):
            part = zf[head * DIM : (head + 1) * DIM, j * 128 : (j + 1) * 128].astype(jnp.float32)
            acc = acc + part * jnp.broadcast_to(alphas[j][head : head + 1, :], (DIM, 128))
        acc = acc + pltpu.roll(acc, ROWS, 1)
        hidden.append(jnp.where(acc > 0, acc, jnp.exp(jnp.minimum(acc, 0.0)) - 1.0))
    hidden = jnp.concatenate(hidden, axis=0)
    hidden = hidden.T[0:ROWS, :].astype(jnp.bfloat16)
    ow_load.wait()
    out[...] = jnp.dot(hidden, ow_in[...], preferred_element_type=jnp.float32).astype(jnp.bfloat16)

    for copy in sends + along:
        copy.wait_send()


def local(
    features, proj_weight, score_src, score_dst, request_rows, slot_index, slot_count, out_weight
):
    vmem = pl.BlockSpec(memory_space=pltpu.VMEM)
    dma = pltpu.SemaphoreType.DMA
    nodes = features.shape[0]
    return pl.pallas_call(
        kernel,
        out_shape=jax.ShapeDtypeStruct((ROWS, OUT), jnp.bfloat16),
        in_specs=[pl.BlockSpec(memory_space=pltpu.HBM)] * 8,
        out_specs=vmem,
        scratch_shapes=[
            pltpu.VMEM((FEAT, nodes), jnp.bfloat16),
            pltpu.VMEM((OWNERS, CAP), jnp.int32),
            pltpu.VMEM((2, 1, DIM), jnp.float32),
            pltpu.VMEM((1, 128), jnp.int32),
            pltpu.VMEM((OUT, OUT), jnp.bfloat16),
            pltpu.VMEM((nodes, 128), jnp.float32),
            pltpu.VMEM((128, 128), jnp.float32),
            pltpu.VMEM((OWNERS * CAP, 128), jnp.float32),
            pltpu.VMEM((OWNERS, 2, PACK, 128), jnp.bfloat16),
            pltpu.VMEM((HALF, 128), jnp.float32),
            pltpu.VMEM((OWNERS, 2, PACK, 128), jnp.bfloat16),
            pltpu.VMEM((HEADS, DIM, FEAT), jnp.bfloat16),
            pltpu.VMEM((HEADS, 2, 128), jnp.float32),
            pltpu.VMEM((SLOTS * ROWS, 128), jnp.float32),
            pltpu.VMEM((OUT, SLOTS * ROWS), jnp.bfloat16),
            pltpu.VMEM((6 * HEADS, OUT), jnp.bfloat16),
            pltpu.SMEM((OWNERS, 2, HALF), jnp.int32),
            pltpu.SMEM((2, HALF), jnp.int32),
            pltpu.SMEM((SLOTS, 128), jnp.int32),
        ]
        + [dma((OWNERS, 2))] * 2
        + [dma((OWNERS,))] * 6
        + [dma((HEADS,))] * 4
        + [dma((10,))],
        compiler_params=pltpu.CompilerParams(
            collective_id=0, has_side_effects=True, vmem_limit_bytes=60 * 1024 * 1024
        ),
        name="layer",
    )(
        features.T, proj_weight.T, score_src, score_dst, request_rows.reshape(OWNERS, CAP),
        slot_index.T, slot_count.reshape(1, -1), out_weight,
    )


def solution(mesh):
    in_specs = (
        P("node", None),
        P(None, "head"),
        P("head", None),
        P("head", None),
        P("node", None, None),
        P("node", None),
        P("node"),
        P(),
    )
    out_specs = P(("node", "head"), None)
    return jax.shard_map(local, mesh=mesh, in_specs=in_specs, out_specs=out_specs, check_vma=False)
```

```python
import functools

import jax
import jax.numpy as jnp
from jax import lax
from jax.experimental import pallas as pl
from jax.experimental.pallas import tpu as pltpu
from jax.sharding import PartitionSpec as P

MESH = pl.DeviceIdType.MESH
RING = (0, 1, 2, 1)
FEAT, HEADS, DIM, OUT, SLOTS = 100, 8, 64, 512, 16
CAP, HALF = 256, 128
PACK = 104
ROWS = 64
OWNERS = 32


def hops(k):
    return RING[k // 8] + RING[(k // 2) % 4]


FAR = sorted((k for k in range(1, OWNERS) if hops(k) >= 2), key=lambda k: (hops(k), -(k % 2), -k))
NEAR = [2, 6, 8, 24, 3, 7, 9, 25, 1]
PEERS = FAR + NEAR
HELD = 0


def shifted(k, sign):
    me = lax.axis_index("node")
    y, x, c = me // 8, (me // 2) % 4, me % 2
    dy, dx, dc = k // 8, (k // 2) % 4, k % 2
    return (((y + sign * dy + 4) % 4) * 4 + (x + sign * dx + 4) % 4) * 2 + (c + sign * dc + 2) % 2


def pack(x):
    lane = lax.broadcasted_iota(jnp.int32, (8, 128), 1)
    group = [x[8 * i : 8 * i + 8] for i in range(16)]
    rows = [jnp.where(lane < 64, group[i], pltpu.roll(group[8 + i], 64, 1)) for i in range(8)]
    for i in range(4):
        acc = group[8 + i]
        for q in (0, 1, 3):
            moved = pltpu.roll(group[4 * q + i], (32 * q - 64) % 128, 1)
            acc = jnp.where(lane // 32 == q, moved, acc)
        rows.append(acc)
    acc = group[12]
    for q in range(16):
        if q != 12:
            acc = jnp.where(lane // 8 == q, pltpu.roll(group[q], (8 * q - 96) % 128, 1), acc)
    rows.append(acc)
    return jnp.concatenate(rows, axis=0)


def unpack(y):
    lane = lax.broadcasted_iota(jnp.int32, (8, 128), 1)
    group = [y[8 * i : 8 * i + 8] for i in range(13)]
    rows = []
    for i in range(16):
        first = group[i] if i < 8 else pltpu.roll(group[i - 8], 64, 1)
        second = group[8 + i % 4]
        if i // 4 != 2:
            second = pltpu.roll(second, (64 - 32 * (i // 4)) % 128, 1)
        third = group[12] if i == 12 else pltpu.roll(group[12], (96 - 8 * i) % 128, 1)
        rows.append(jnp.where(lane < 64, first, jnp.where(lane < 96, second, third)))
    return jnp.concatenate(rows, axis=0)


def kernel(
    feat_t, w_t, s_src, s_dst, req, slot_t, cnt, ow, out,
    feat_in, req_in, sc_in, cnt_in, ow_in,
    feat, blk, tab, rx, stage, sendbuf, w_all, sc_all, gath, zf, sc_mat, req_sm, own_sm, slot_sm,
    rq_s, rq_r, rw_s, rw_r, up_s, up_r, dn_s, dn_r, w_s, w_r, sc_s, sc_r, loc,
):
    me, h = lax.axis_index("node"), lax.axis_index("head")
    half = h % 2
    up, down = (h + 1) % HEADS, (h + HEADS - 1) % HEADS

    barrier = pltpu.get_barrier_semaphore()
    for k in PEERS:
        pl.semaphore_signal(barrier, inc=1, device_id=(shifted(k, 1), h), device_id_type=MESH)
    for z in range(1, HEADS):
        pl.semaphore_signal(barrier, inc=1, device_id=(me, (h + z) % HEADS), device_id_type=MESH)

    lane_block = pl.multiple_of(h // 2 * 128, 128)
    loads = [
        pltpu.make_async_copy(src, dst, loc.at[n])
        for n, (src, dst) in enumerate(
            (
                (feat_t, feat_in),
                (req, req_in),
                (req.at[me, pl.ds(0, HALF)], own_sm.at[0]),
                (req.at[me, pl.ds(HALF, HALF)], own_sm.at[1]),
                (w_t, w_all.at[h]),
                (s_src, sc_in.at[0]),
                (s_dst, sc_in.at[1]),
                (slot_t.at[:, pl.ds(lane_block, 128)], slot_sm),
                (cnt.at[:, pl.ds(lane_block, 128)], cnt_in),
                (ow, ow_in),
            )
        )
    ]
    for load in loads:
        load.start()
    feat_load, req_load, own_load, own_load2, w_load, src_load, dst_load, slot_load, cnt_load, ow_load = loads

    blk[...] = jnp.zeros_like(blk)
    feat_load.wait()
    for j in range(feat.shape[0] // 128):
        blk[0:FEAT, :] = feat_in[:, j * 128 : (j + 1) * 128].astype(jnp.float32)
        feat[j * 128 : (j + 1) * 128, :] = blk[...].T
    src_load.wait()
    dst_load.wait()
    both = jnp.concatenate([sc_in[0], sc_in[1]], axis=0)
    sc_all[h] = jnp.concatenate([both, both], axis=1)
    w_load.wait()
    req_load.wait()

    pl.semaphore_wait(barrier, OWNERS - 1 + HEADS - 1)

    def ask(k, part, owner, target):
        column = half if k in FAR else part
        return pltpu.make_async_remote_copy(
            src_ref=req_in.at[owner, pl.ds(pl.multiple_of(column * HALF, HALF), HALF)],
            dst_ref=req_sm.at[k, part],
            send_sem=rq_s.at[k, part], recv_sem=rq_r.at[k, part],
            device_id=(target, h), device_id_type=MESH,
        )

    sends = []
    for k in PEERS:
        owner = shifted(k, -1)
        for part in range(1 if k in FAR else 2):
            copy = ask(k, part, owner, owner)
            copy.start()
            sends.append(copy)
    along = []
    for z in range(1, HEADS):
        peer = (me, (h + z) % HEADS)
        copy = pltpu.make_async_remote_copy(
            src_ref=w_all.at[h], dst_ref=w_all.at[h], send_sem=w_s.at[z], recv_sem=w_r.at[z],
            device_id=peer, device_id_type=MESH,
        )
        copy.start()
        along.append(copy)
        copy = pltpu.make_async_remote_copy(
            src_ref=sc_all.at[h], dst_ref=sc_all.at[h], send_sem=sc_s.at[z], recv_sem=sc_r.at[z],
            device_id=peer, device_id_type=MESH,
        )
        copy.start()
        along.append(copy)

    def pick(table, number, target, base, count):
        for u in range(count):
            target[pl.ds(base + u, 1), :] = table[pl.ds(number(u), 1), :]

    own_load.wait()
    own_load2.wait()

    def own(part, carry):
        pick(feat, lambda u: own_sm[part, u], tab, me * CAP + part * HALF, HALF)
        return carry

    lax.fori_loop(0, 2, own, 0)

    def give(k):
        src, dst = (sendbuf.at[k, 0], rx.at[k, half]) if k in FAR else (sendbuf.at[k], rx.at[k])
        return pltpu.make_async_remote_copy(
            src_ref=src, dst_ref=dst, send_sem=rw_s.at[k],
            recv_sem=rw_r.at[k], device_id=(shifted(k, 1), h), device_id_type=MESH,
        )

    def send(k):
        copy = give(k)
        copy.start()
        sends.append(copy)

    def serve(k):
        parts = 1 if k in FAR else 2
        for part in range(parts):
            ask(k, part, 0, shifted(k, 1)).wait_recv()

        def some(part, carry):
            pick(feat, lambda u: req_sm[k, part, u], stage, 0, HALF)
            sendbuf[k, part] = pack(stage[...]).astype(jnp.bfloat16)
            return carry

        lax.fori_loop(0, parts, some, 0)
        send(k)

    for k in FAR:
        serve(k)

    def spread(k, part):
        place = pl.multiple_of(shifted(k, -1) * CAP + part * HALF, HALF)
        tab[pl.ds(place, HALF), :] = unpack(rx[k, part].astype(jnp.float32))

    def hand(k, part, mine, first):
        start, count = (0, 48) if first == FAR.index(k) % 2 else (48, PACK - 48)
        ref = rx.at[k, mine, pl.ds(start, count)]
        sem = (up_s, up_r) if first == 0 else (dn_s, dn_r)
        return pltpu.make_async_remote_copy(
            src_ref=ref, dst_ref=ref, send_sem=sem[0].at[k], recv_sem=sem[1].at[k],
            device_id=(me, part), device_id_type=MESH,
        )

    for n, k in enumerate(FAR):
        give(k).wait_recv()
        for part, first in ((up, 0), (down, 1)):
            copy = hand(k, part, half, first)
            copy.start()
            along.append(copy)
        spread(k, half)
        if HELD <= n < HELD + len(NEAR):
            serve(NEAR[n - HELD])
    for z in range(1, HEADS):
        other = (h + HEADS - z) % HEADS
        pltpu.make_async_remote_copy(
            src_ref=w_all.at[h], dst_ref=w_all.at[other], send_sem=w_s.at[z], recv_sem=w_r.at[z],
            device_id=(me, up), device_id_type=MESH,
        ).wait_recv()
        pltpu.make_async_remote_copy(
            src_ref=sc_all.at[h], dst_ref=sc_all.at[other], send_sem=sc_s.at[z],
            recv_sem=sc_r.at[z], device_id=(me, up), device_id_type=MESH,
        ).wait_recv()

    row = lax.broadcasted_iota(jnp.int32, (2 * HEADS, OUT), 0)
    lane = lax.broadcasted_iota(jnp.int32, (2 * HEADS, OUT), 1)
    score = jnp.zeros((2 * HEADS, OUT), jnp.float32)
    for head in range(HEADS):
        for which in range(2):
            vec = sc_all[head, which : which + 1, :]
            vec = jnp.broadcast_to(jnp.concatenate([vec] * 4, axis=1), (2 * HEADS, OUT))
            hit = (row == which * HEADS + head) & (lane // DIM == head)
            score = jnp.where(hit, vec, score)
    top = score.astype(jnp.bfloat16)
    rest = score - top.astype(jnp.float32)
    mid = rest.astype(jnp.bfloat16)
    low = (rest - mid.astype(jnp.float32)).astype(jnp.bfloat16)
    for n, piece in enumerate((top, mid, low)):
        sc_mat[n * 2 * HEADS : (n + 1) * 2 * HEADS, :] = piece

    for k in NEAR:
        give(k).wait_recv()

        def both_halves(part, carry, k=k):
            spread(k, part)
            return carry

        lax.fori_loop(0, 2, both_halves, 0)
    for copy in sends + along:
        copy.wait_send()
    for k in FAR:
        hand(k, down, 1 - half, 0).wait_recv()
        hand(k, up, 1 - half, 1).wait_recv()
        spread(k, 1 - half)
    slot_load.wait()
    for side in range(2):

        @pl.when(half == side)
        def _(side=side):
            def some(s, carry):
                pick(tab, lambda u: slot_sm[s, side * ROWS + u], gath, s * ROWS, ROWS)
                return carry

            lax.fori_loop(0, SLOTS, some, 0)

    g = gath[...][:, 0:FEAT].astype(jnp.bfloat16)
    zf[...] = lax.dot_general(
        w_all[...].reshape(OUT, FEAT), g, (((1,), (1,)), ((), ())),
        preferred_element_type=jnp.float32,
    ).astype(jnp.bfloat16)
    parts = jnp.dot(sc_mat[...], zf[...], preferred_element_type=jnp.float32)
    total = parts[0:16] + parts[16:32] + parts[32:48]
    n = SLOTS * ROWS // 128
    lanes = lax.broadcasted_iota(jnp.int32, (HEADS, 128), 1)
    dst_part = total[HEADS:, 0:128]
    dst_part = jnp.where(lanes < ROWS, dst_part, pltpu.roll(dst_part, ROWS, 1))
    cnt_load.wait()
    pair = jnp.broadcast_to(cnt_in[...], (HEADS, 128))
    turned = pltpu.roll(pair, ROWS, 1)
    counts = jnp.where((lanes // ROWS) == half, pair, turned)
    logits, lives = [], []
    for j in range(n):
        logit = total[0:HEADS, j * 128 : (j + 1) * 128] + dst_part
        logit = jnp.where(logit > 0, logit, 0.2 * logit)
        live = (2 * j + lanes // ROWS) < counts
        logits.append(jnp.where(live, logit, -1e30))
        lives.append(live)
    peak = functools.reduce(jnp.maximum, logits)
    peak = jnp.maximum(peak, pltpu.roll(peak, ROWS, 1))
    weights = [
        jnp.where(live, jnp.exp(logit - peak), 0.0) for live, logit in zip(lives, logits)
    ]
    norm = functools.reduce(jnp.add, weights)
    norm = norm + pltpu.roll(norm, ROWS, 1)
    alphas = [(w / norm).astype(jnp.bfloat16).astype(jnp.float32) for w in weights]
    hidden = []
    for head in range(HEADS):
        acc = jnp.zeros((DIM, 128), jnp.float32)
        for j in range(n):
            part = zf[head * DIM : (head + 1) * DIM, j * 128 : (j + 1) * 128].astype(jnp.float32)
            acc = acc + part * jnp.broadcast_to(alphas[j][head : head + 1, :], (DIM, 128))
        acc = acc + pltpu.roll(acc, ROWS, 1)
        hidden.append(jnp.where(acc > 0, acc, jnp.exp(jnp.minimum(acc, 0.0)) - 1.0))
    hidden = jnp.concatenate(hidden, axis=0)
    hidden = hidden.T[0:ROWS, :].astype(jnp.bfloat16)
    ow_load.wait()
    out[...] = jnp.dot(hidden, ow_in[...], preferred_element_type=jnp.float32).astype(jnp.bfloat16)


def local(
    features, proj_weight, score_src, score_dst, request_rows, slot_index, slot_count, out_weight
):
    vmem = pl.BlockSpec(memory_space=pltpu.VMEM)
    dma = pltpu.SemaphoreType.DMA
    nodes = features.shape[0]
    return pl.pallas_call(
        kernel,
        out_shape=jax.ShapeDtypeStruct((ROWS, OUT), jnp.bfloat16),
        in_specs=[pl.BlockSpec(memory_space=pltpu.HBM)] * 8,
        out_specs=vmem,
        scratch_shapes=[
            pltpu.VMEM((FEAT, nodes), jnp.bfloat16),
            pltpu.VMEM((OWNERS, CAP), jnp.int32),
            pltpu.VMEM((2, 1, DIM), jnp.float32),
            pltpu.VMEM((1, 128), jnp.int32),
            pltpu.VMEM((OUT, OUT), jnp.bfloat16),
            pltpu.VMEM((nodes, 128), jnp.float32),
            pltpu.VMEM((128, 128), jnp.float32),
            pltpu.VMEM((OWNERS * CAP, 128), jnp.float32),
            pltpu.VMEM((OWNERS, 2, PACK, 128), jnp.bfloat16),
            pltpu.VMEM((HALF, 128), jnp.float32),
            pltpu.VMEM((OWNERS, 2, PACK, 128), jnp.bfloat16),
            pltpu.VMEM((HEADS, DIM, FEAT), jnp.bfloat16),
            pltpu.VMEM((HEADS, 2, 128), jnp.float32),
            pltpu.VMEM((SLOTS * ROWS, 128), jnp.float32),
            pltpu.VMEM((OUT, SLOTS * ROWS), jnp.bfloat16),
            pltpu.VMEM((6 * HEADS, OUT), jnp.bfloat16),
            pltpu.SMEM((OWNERS, 2, HALF), jnp.int32),
            pltpu.SMEM((2, HALF), jnp.int32),
            pltpu.SMEM((SLOTS, 128), jnp.int32),
        ]
        + [dma((OWNERS, 2))] * 2
        + [dma((OWNERS,))] * 6
        + [dma((HEADS,))] * 4
        + [dma((10,))],
        compiler_params=pltpu.CompilerParams(
            collective_id=0, has_side_effects=True, vmem_limit_bytes=60 * 1024 * 1024
        ),
        name="layer",
    )(
        features.T, proj_weight.T, score_src, score_dst, request_rows.reshape(OWNERS, CAP),
        slot_index.T, slot_count.reshape(1, -1), out_weight,
    )


def solution(mesh):
    in_specs = (
        P("node", None),
        P(None, "head"),
        P("head", None),
        P("head", None),
        P("node", None, None),
        P("node", None),
        P("node"),
        P(),
    )
    out_specs = P(("node", "head"), None)
    return jax.shard_map(local, mesh=mesh, in_specs=in_specs, out_specs=out_specs, check_vma=False)
```

```python
import functools

import jax
import jax.numpy as jnp
from jax import lax
from jax.experimental import pallas as pl
from jax.experimental.pallas import tpu as pltpu
from jax.sharding import PartitionSpec as P

MESH = pl.DeviceIdType.MESH
RING = (0, 1, 2, 1)
FEAT, HEADS, DIM, OUT, SLOTS = 100, 8, 64, 512, 16
CAP, HALF = 256, 128
PACK = 104
ROWS = 64
OWNERS = 32


def hops(k):
    return RING[k // 8] + RING[(k // 2) % 4]


FAR = sorted((k for k in range(1, OWNERS) if hops(k) >= 2), key=lambda k: (hops(k), -(k % 2), -k))
NEAR = [2, 6, 8, 24, 3, 7, 9, 25, 1]
PEERS = FAR + NEAR
HELD = 0


def shifted(k, sign):
    me = lax.axis_index("node")
    y, x, c = me // 8, (me // 2) % 4, me % 2
    dy, dx, dc = k // 8, (k // 2) % 4, k % 2
    return (((y + sign * dy + 4) % 4) * 4 + (x + sign * dx + 4) % 4) * 2 + (c + sign * dc + 2) % 2


def pack(x):
    lane = lax.broadcasted_iota(jnp.int32, (8, 128), 1)
    group = [x[8 * i : 8 * i + 8] for i in range(16)]
    rows = [jnp.where(lane < 64, group[i], pltpu.roll(group[8 + i], 64, 1)) for i in range(8)]
    for i in range(4):
        acc = group[8 + i]
        for q in (0, 1, 3):
            moved = pltpu.roll(group[4 * q + i], (32 * q - 64) % 128, 1)
            acc = jnp.where(lane // 32 == q, moved, acc)
        rows.append(acc)
    acc = group[12]
    for q in range(16):
        if q != 12:
            acc = jnp.where(lane // 8 == q, pltpu.roll(group[q], (8 * q - 96) % 128, 1), acc)
    rows.append(acc)
    return jnp.concatenate(rows, axis=0)


def unpack(y):
    lane = lax.broadcasted_iota(jnp.int32, (8, 128), 1)
    group = [y[8 * i : 8 * i + 8] for i in range(13)]
    rows = []
    for i in range(16):
        first = group[i] if i < 8 else pltpu.roll(group[i - 8], 64, 1)
        second = group[8 + i % 4]
        if i // 4 != 2:
            second = pltpu.roll(second, (64 - 32 * (i // 4)) % 128, 1)
        third = group[12] if i == 12 else pltpu.roll(group[12], (96 - 8 * i) % 128, 1)
        rows.append(jnp.where(lane < 64, first, jnp.where(lane < 96, second, third)))
    return jnp.concatenate(rows, axis=0)


def kernel(
    feat_t, w_t, s_src, s_dst, req, slot_t, cnt, ow, out,
    feat_in, req_in, sc_in, cnt_in, ow_in,
    feat, blk, tab, rx, stage, sendbuf, w_all, sc_all, gath, zf, sc_mat, req_sm, own_sm, slot_sm,
    rq_s, rq_r, rw_s, rw_r, up_s, up_r, dn_s, dn_r, w_s, w_r, sc_s, sc_r, loc,
):
    me, h = lax.axis_index("node"), lax.axis_index("head")
    half = h % 2
    up, down = (h + 1) % HEADS, (h + HEADS - 1) % HEADS

    barrier = pltpu.get_barrier_semaphore()
    for k in PEERS:
        pl.semaphore_signal(barrier, inc=1, device_id=(shifted(k, 1), h), device_id_type=MESH)
    for z in range(1, HEADS):
        pl.semaphore_signal(barrier, inc=1, device_id=(me, (h + z) % HEADS), device_id_type=MESH)

    lane_block = pl.multiple_of(h // 2 * 128, 128)
    loads = [
        pltpu.make_async_copy(src, dst, loc.at[n])
        for n, (src, dst) in enumerate(
            (
                (feat_t, feat_in),
                (req, req_in),
                (req.at[me, pl.ds(0, HALF)], own_sm.at[0]),
                (req.at[me, pl.ds(HALF, HALF)], own_sm.at[1]),
                (w_t, w_all.at[h]),
                (s_src, sc_in.at[0]),
                (s_dst, sc_in.at[1]),
                (slot_t.at[:, pl.ds(lane_block, 128)], slot_sm),
                (cnt.at[:, pl.ds(lane_block, 128)], cnt_in),
                (ow, ow_in),
            )
        )
    ]
    for load in loads:
        load.start()
    feat_load, req_load, own_load, own_load2, w_load, src_load, dst_load, slot_load, cnt_load, ow_load = loads

    blk[...] = jnp.zeros_like(blk)
    feat_load.wait()
    for j in range(feat.shape[0] // 128):
        blk[0:FEAT, :] = feat_in[:, j * 128 : (j + 1) * 128].astype(jnp.float32)
        feat[j * 128 : (j + 1) * 128, :] = blk[...].T
    src_load.wait()
    dst_load.wait()
    both = jnp.concatenate([sc_in[0], sc_in[1]], axis=0)
    sc_all[h] = jnp.concatenate([both, both], axis=1)
    w_load.wait()
    req_load.wait()

    pl.semaphore_wait(barrier, OWNERS - 1 + HEADS - 1)

    def ask(k, part, owner, target):
        column = half if k in FAR else part
        return pltpu.make_async_remote_copy(
            src_ref=req_in.at[owner, pl.ds(pl.multiple_of(column * HALF, HALF), HALF)],
            dst_ref=req_sm.at[k, part],
            send_sem=rq_s.at[k, part], recv_sem=rq_r.at[k, part],
            device_id=(target, h), device_id_type=MESH,
        )

    sends = []
    for k in PEERS:
        owner = shifted(k, -1)
        for part in range(1 if k in FAR else 2):
            copy = ask(k, part, owner, owner)
            copy.start()
            sends.append(copy)
    along = []
    for z in range(1, HEADS):
        peer = (me, (h + z) % HEADS)
        copy = pltpu.make_async_remote_copy(
            src_ref=w_all.at[h], dst_ref=w_all.at[h], send_sem=w_s.at[z], recv_sem=w_r.at[z],
            device_id=peer, device_id_type=MESH,
        )
        copy.start()
        along.append(copy)
        copy = pltpu.make_async_remote_copy(
            src_ref=sc_all.at[h], dst_ref=sc_all.at[h], send_sem=sc_s.at[z], recv_sem=sc_r.at[z],
            device_id=peer, device_id_type=MESH,
        )
        copy.start()
        along.append(copy)

    def pick(table, number, target, base, count):
        for u in range(count):
            target[pl.ds(base + u, 1), :] = table[pl.ds(number(u), 1), :]

    own_load.wait()
    own_load2.wait()

    def own(part, carry):
        pick(feat, lambda u: own_sm[part, u], tab, me * CAP + part * HALF, HALF)
        return carry

    lax.fori_loop(0, 2, own, 0)

    def give(k):
        src, dst = (sendbuf.at[k, 0], rx.at[k, half]) if k in FAR else (sendbuf.at[k], rx.at[k])
        return pltpu.make_async_remote_copy(
            src_ref=src, dst_ref=dst, send_sem=rw_s.at[k],
            recv_sem=rw_r.at[k], device_id=(shifted(k, 1), h), device_id_type=MESH,
        )

    def send(k):
        copy = give(k)
        copy.start()
        sends.append(copy)

    def serve(k):
        parts = 1 if k in FAR else 2
        for part in range(parts):
            ask(k, part, 0, shifted(k, 1)).wait_recv()

        def some(part, carry):
            pick(feat, lambda u: req_sm[k, part, u], stage, 0, HALF)
            sendbuf[k, part] = pack(stage[...]).astype(jnp.bfloat16)
            return carry

        lax.fori_loop(0, parts, some, 0)
        send(k)

    serve(NEAR[-1])
    for k in FAR:
        serve(k)

    def spread(k, part):
        place = pl.multiple_of(shifted(k, -1) * CAP + part * HALF, HALF)
        tab[pl.ds(place, HALF), :] = unpack(rx[k, part].astype(jnp.float32))

    def hand(k, part, mine, first):
        start, count = (0, 48) if first == FAR.index(k) % 2 else (48, PACK - 48)
        ref = rx.at[k, mine, pl.ds(start, count)]
        sem = (up_s, up_r) if first == 0 else (dn_s, dn_r)
        return pltpu.make_async_remote_copy(
            src_ref=ref, dst_ref=ref, send_sem=sem[0].at[k], recv_sem=sem[1].at[k],
            device_id=(me, part), device_id_type=MESH,
        )

    for n, k in enumerate(FAR):
        give(k).wait_recv()
        for part, first in ((up, 0), (down, 1)):
            copy = hand(k, part, half, first)
            copy.start()
            along.append(copy)
        spread(k, half)
        if HELD <= n < HELD + len(NEAR) - 1:
            serve(NEAR[n - HELD])
    for z in range(1, HEADS):
        other = (h + HEADS - z) % HEADS
        pltpu.make_async_remote_copy(
            src_ref=w_all.at[h], dst_ref=w_all.at[other], send_sem=w_s.at[z], recv_sem=w_r.at[z],
            device_id=(me, up), device_id_type=MESH,
        ).wait_recv()
        pltpu.make_async_remote_copy(
            src_ref=sc_all.at[h], dst_ref=sc_all.at[other], send_sem=sc_s.at[z],
            recv_sem=sc_r.at[z], device_id=(me, up), device_id_type=MESH,
        ).wait_recv()

    row = lax.broadcasted_iota(jnp.int32, (2 * HEADS, OUT), 0)
    lane = lax.broadcasted_iota(jnp.int32, (2 * HEADS, OUT), 1)
    score = jnp.zeros((2 * HEADS, OUT), jnp.float32)
    for head in range(HEADS):
        for which in range(2):
            vec = sc_all[head, which : which + 1, :]
            vec = jnp.broadcast_to(jnp.concatenate([vec] * 4, axis=1), (2 * HEADS, OUT))
            hit = (row == which * HEADS + head) & (lane // DIM == head)
            score = jnp.where(hit, vec, score)
    top = score.astype(jnp.bfloat16)
    rest = score - top.astype(jnp.float32)
    mid = rest.astype(jnp.bfloat16)
    low = (rest - mid.astype(jnp.float32)).astype(jnp.bfloat16)
    for n, piece in enumerate((top, mid, low)):
        sc_mat[n * 2 * HEADS : (n + 1) * 2 * HEADS, :] = piece

    for k in NEAR:
        give(k).wait_recv()

        def both_halves(part, carry, k=k):
            spread(k, part)
            return carry

        lax.fori_loop(0, 2, both_halves, 0)
    for copy in sends + along:
        copy.wait_send()
    for k in FAR:
        hand(k, down, 1 - half, 0).wait_recv()
        hand(k, up, 1 - half, 1).wait_recv()
        spread(k, 1 - half)
    slot_load.wait()
    for side in range(2):

        @pl.when(half == side)
        def _(side=side):
            def some(s, carry):
                pick(tab, lambda u: slot_sm[s, side * ROWS + u], gath, s * ROWS, ROWS)
                return carry

            lax.fori_loop(0, SLOTS, some, 0)

    g = gath[...][:, 0:FEAT].astype(jnp.bfloat16)
    zf[...] = lax.dot_general(
        w_all[...].reshape(OUT, FEAT), g, (((1,), (1,)), ((), ())),
        preferred_element_type=jnp.float32,
    ).astype(jnp.bfloat16)
    parts = jnp.dot(sc_mat[...], zf[...], preferred_element_type=jnp.float32)
    total = parts[0:16] + parts[16:32] + parts[32:48]
    n = SLOTS * ROWS // 128
    lanes = lax.broadcasted_iota(jnp.int32, (HEADS, 128), 1)
    dst_part = total[HEADS:, 0:128]
    dst_part = jnp.where(lanes < ROWS, dst_part, pltpu.roll(dst_part, ROWS, 1))
    cnt_load.wait()
    pair = jnp.broadcast_to(cnt_in[...], (HEADS, 128))
    turned = pltpu.roll(pair, ROWS, 1)
    counts = jnp.where((lanes // ROWS) == half, pair, turned)
    logits, lives = [], []
    for j in range(n):
        logit = total[0:HEADS, j * 128 : (j + 1) * 128] + dst_part
        logit = jnp.where(logit > 0, logit, 0.2 * logit)
        live = (2 * j + lanes // ROWS) < counts
        logits.append(jnp.where(live, logit, -1e30))
        lives.append(live)
    peak = functools.reduce(jnp.maximum, logits)
    peak = jnp.maximum(peak, pltpu.roll(peak, ROWS, 1))
    weights = [
        jnp.where(live, jnp.exp(logit - peak), 0.0) for live, logit in zip(lives, logits)
    ]
    norm = functools.reduce(jnp.add, weights)
    norm = norm + pltpu.roll(norm, ROWS, 1)
    alphas = [(w / norm).astype(jnp.bfloat16).astype(jnp.float32) for w in weights]
    hidden = []
    for head in range(HEADS):
        acc = jnp.zeros((DIM, 128), jnp.float32)
        for j in range(n):
            part = zf[head * DIM : (head + 1) * DIM, j * 128 : (j + 1) * 128].astype(jnp.float32)
            acc = acc + part * jnp.broadcast_to(alphas[j][head : head + 1, :], (DIM, 128))
        acc = acc + pltpu.roll(acc, ROWS, 1)
        hidden.append(jnp.where(acc > 0, acc, jnp.exp(jnp.minimum(acc, 0.0)) - 1.0))
    hidden = jnp.concatenate(hidden, axis=0)
    hidden = hidden.T[0:ROWS, :].astype(jnp.bfloat16)
    ow_load.wait()
    out[...] = jnp.dot(hidden, ow_in[...], preferred_element_type=jnp.float32).astype(jnp.bfloat16)


def local(
    features, proj_weight, score_src, score_dst, request_rows, slot_index, slot_count, out_weight
):
    vmem = pl.BlockSpec(memory_space=pltpu.VMEM)
    dma = pltpu.SemaphoreType.DMA
    nodes = features.shape[0]
    return pl.pallas_call(
        kernel,
        out_shape=jax.ShapeDtypeStruct((ROWS, OUT), jnp.bfloat16),
        in_specs=[pl.BlockSpec(memory_space=pltpu.HBM)] * 8,
        out_specs=vmem,
        scratch_shapes=[
            pltpu.VMEM((FEAT, nodes), jnp.bfloat16),
            pltpu.VMEM((OWNERS, CAP), jnp.int32),
            pltpu.VMEM((2, 1, DIM), jnp.float32),
            pltpu.VMEM((1, 128), jnp.int32),
            pltpu.VMEM((OUT, OUT), jnp.bfloat16),
            pltpu.VMEM((nodes, 128), jnp.float32),
            pltpu.VMEM((128, 128), jnp.float32),
            pltpu.VMEM((OWNERS * CAP, 128), jnp.float32),
            pltpu.VMEM((OWNERS, 2, PACK, 128), jnp.bfloat16),
            pltpu.VMEM((HALF, 128), jnp.float32),
            pltpu.VMEM((OWNERS, 2, PACK, 128), jnp.bfloat16),
            pltpu.VMEM((HEADS, DIM, FEAT), jnp.bfloat16),
            pltpu.VMEM((HEADS, 2, 128), jnp.float32),
            pltpu.VMEM((SLOTS * ROWS, 128), jnp.float32),
            pltpu.VMEM((OUT, SLOTS * ROWS), jnp.bfloat16),
            pltpu.VMEM((6 * HEADS, OUT), jnp.bfloat16),
            pltpu.SMEM((OWNERS, 2, HALF), jnp.int32),
            pltpu.SMEM((2, HALF), jnp.int32),
            pltpu.SMEM((SLOTS, 128), jnp.int32),
        ]
        + [dma((OWNERS, 2))] * 2
        + [dma((OWNERS,))] * 6
        + [dma((HEADS,))] * 4
        + [dma((10,))],
        compiler_params=pltpu.CompilerParams(
            collective_id=0, has_side_effects=True, vmem_limit_bytes=60 * 1024 * 1024
        ),
        name="layer",
    )(
        features.T, proj_weight.T, score_src, score_dst, request_rows.reshape(OWNERS, CAP),
        slot_index.T, slot_count.reshape(1, -1), out_weight,
    )


def solution(mesh):
    in_specs = (
        P("node", None),
        P(None, "head"),
        P("head", None),
        P("head", None),
        P("node", None, None),
        P("node", None),
        P("node"),
        P(),
    )
    out_specs = P(("node", "head"), None)
    return jax.shard_map(local, mesh=mesh, in_specs=in_specs, out_specs=out_specs, check_vma=False)
```
